256 devices in a mesh: samp: 4 (over y), var: 64 (over x, z, core).
Axes of the slice: x: 4, y: 4, z: 8, core: 2. Of those that a mesh axis runs over, the one named last changes fastest.
Arguments:
- samples: bfloat16 [1024, 262144], P('samp', 'var'), may hold values from -6 to 6
- precision_blocks: bfloat16 [1024, 3, 256, 256], P('var'), may hold values from -6 to 6
- pair_rows: int32 [1024, 3], P('var'), may hold values from 0 to 1023, as said below
Outputs:
- gradient: float32 [1024, 3, 256, 256], P('var', None, 'samp')
The draws below stay inside these ranges and needn't reach their ends.
Inputs may be any that keep to these rules, and one draw needn't show every extreme that they name: pair_rows[j, 0] = j. For k >= 1, pair_rows[j, k] = j XOR (16 * c) with c a nonzero value below the number of indices of var that depends only on k and j mod 16, so pair_rows[pair_rows[j, k], k] = j. Over the off-diagonal slots of the blocks of one index of var, at most 1 partners lie on any one other index, and some pair of indices reaches 1.
All inputs are finite; a program needn't handle non-finite values.
Results may differ from the reference program's by a relative error of at most 0.0019.
Values may be sent and summed in bfloat16 or wider, within the bound.
A program may use at most 128 MiB of HBM per device.

```python
import jax
import jax.numpy as jnp
from jax import lax

BS = 256
KB = 16
R = 3
NBLK = 1024
P_SIZE = 262144
NSAMP = 1024


def draw_pair_rows(key, part):
    var_count = NBLK // KB
    levels = R - 1
    half_value = var_count // 2
    key_first = jax.random.fold_in(key, 11)
    key_second = jax.random.fold_in(key, 23)
    if var_count == 2:
        values_order = jnp.ones((1,), jnp.int32)
    else:
        rest = jax.random.permutation(key_first, var_count - 3).astype(jnp.int32) + 2
        rest = jnp.where(rest >= half_value, rest + 1, rest)
        values_order = jnp.concatenate([jnp.full((1,), half_value, jnp.int32), jnp.ones((1,), jnp.int32), rest])
    repeats = -(-(levels * KB) // (var_count - 1))
    tiled = jnp.tile(values_order, repeats)[:levels * KB]
    shuffled = jax.random.permutation(key_second, tiled)
    xor_values = shuffled.reshape(levels, KB).astype(jnp.int32)
    block_ids = jnp.arange(NBLK, dtype=jnp.int32)
    local_index = block_ids % KB
    owner_index = block_ids // KB
    columns = [block_ids]
    for level in range(levels):
        partner_owner = jnp.bitwise_xor(owner_index, xor_values[level][local_index])
        columns.append(partner_owner * KB + local_index)
    return jnp.stack(columns, axis=1).astype(jnp.int32)


def level_of(stream_key, dims, split, least, high):
    gain, own = 1.0, jax.random.fold_in(stream_key, 6)
    for dim, blocks in split:
        heights = jnp.exp(jax.random.uniform(jax.random.fold_in(own, dim), (blocks,), jnp.float32, least / len(split), high / len(split)))
        gain = gain * jnp.repeat(heights, dims[dim] // blocks).reshape([-1 if axis == dim else 1 for axis in range(len(dims))])
    return gain


def noise(own_key, dims, deviation, limit, split=(), held_as=jnp.bfloat16):
    drawn = jax.random.normal(own_key, dims, jnp.float32) * deviation
    if len(split) > 0:
        drawn = level_of(own_key, dims, split, -0.22, 0.18) * drawn
    return jnp.clip(drawn, min=-limit, max=limit).astype(held_as)


def setup_inputs(seed: int = 0) -> dict:
    streams_of = jax.random.split(jax.random.key(seed), 4)
    samples = noise(streams_of[0], (NSAMP, P_SIZE), 1.0, 6.0, ((0, 4), (1, 64)))
    precision_blocks = noise(streams_of[1], (NBLK, R, BS, BS), 1.0, 6.0, ((0, 64),))
    pair_rows = draw_pair_rows(jax.random.fold_in(streams_of[3], 71), 0)
    return {"samples": samples, "precision_blocks": precision_blocks, "pair_rows": pair_rows}


def reference(samples, precision_blocks, pair_rows):
    column_view = samples.reshape(NSAMP, NBLK, BS)

    def mix_column(col_id):
        partner_ids = pair_rows[col_id]
        running = jnp.zeros((NSAMP, BS), jnp.float32)
        for slot in range(R):
            running = running + jnp.dot(column_view[:, partner_ids[slot], :], precision_blocks[col_id, slot], preferred_element_type=jnp.float32)
        return running.astype(jnp.bfloat16)

    mixed_cols = lax.map(mix_column, jnp.arange(NBLK, dtype=jnp.int32))

    def grad_column(col_id):
        partner_ids = pair_rows[col_id]
        own_cols = column_view[:, col_id, :]
        own_mixed = mixed_cols[col_id]
        pieces = []
        for slot in range(R):
            row_id = partner_ids[slot]
            own_term = jnp.dot(column_view[:, row_id, :].T, own_mixed, preferred_element_type=jnp.float32)
            other_term = jnp.dot(mixed_cols[row_id].T, own_cols, preferred_element_type=jnp.float32)
            pieces.append((own_term + other_term) * (0.5 / NSAMP))
        return jnp.stack(pieces)

    return lax.map(grad_column, jnp.arange(NBLK, dtype=jnp.int32))
```

```python
import jax
import jax.numpy as jnp
from jax import lax
from jax.experimental import pallas as pl
from jax.experimental.pallas import tpu as pltpu
from jax.sharding import PartitionSpec as P


def pick_columns(columns, samples, width, group):
    rows, total = samples.shape
    count = columns.shape[0]
    group = min(group, count)

    def body(index_ref, x_ref, o_ref):
        first = pl.program_id(0) * group
        for i in range(group):
            start = pl.multiple_of(index_ref[first + i] * width, width)
            o_ref[i] = x_ref[:, pl.ds(start, width)]

    return pl.pallas_call(
        body,
        out_shape=jax.ShapeDtypeStruct((count, rows, width), samples.dtype),
        grid_spec=pltpu.PrefetchScalarGridSpec(
            num_scalar_prefetch=1,
            grid=(count // group,),
            in_specs=[pl.BlockSpec((rows, total), lambda g, index: (0, 0))],
            out_specs=pl.BlockSpec((group, rows, width), lambda g, index: (g, 0, 0)),
        ),
        name="pick_columns",
    )(columns, samples)


def pick_blocks(picked, blocks, group):
    _, rows, width = blocks.shape
    count = picked.shape[0]
    group = min(group, count)

    def body(index_ref, *refs):
        for i in range(group):
            refs[group][i] = refs[i][0]

    def source(i):
        return pl.BlockSpec((1, rows, width), lambda g, index: (index[g * group + i], 0, 0))

    return pl.pallas_call(
        body,
        out_shape=jax.ShapeDtypeStruct((count, rows, width), blocks.dtype),
        grid_spec=pltpu.PrefetchScalarGridSpec(
            num_scalar_prefetch=1,
            grid=(count // group,),
            in_specs=[source(i) for i in range(group)],
            out_specs=pl.BlockSpec((group, rows, width), lambda g, index: (g, 0, 0)),
        ),
        name="pick_blocks",
    )(picked, *([blocks] * group))


def gradient_terms(group_index, own, fetched, precision, norm_factor):
    chunks, per_group, rows, width = own.shape
    levels = fetched.shape[1]
    slots = levels + 1
    part = width // chunks

    def body(index_ref, own_ref, fetched_ref, p_ref, rows_ref, turned_ref):
        totals = [jnp.zeros((width, width), jnp.float32) for _ in range(slots)]
        for s in range(chunks):
            factors = [own_ref[s, 0]] + [fetched_ref[s, k, 0] for k in range(levels)]
            mixed = jnp.zeros((rows, width), jnp.float32)
            for k in range(slots):
                mixed = mixed + jnp.dot(factors[k], p_ref[0, k], preferred_element_type=jnp.float32)
            mixed = mixed.astype(jnp.bfloat16)
            for k in range(slots):
                totals[k] = totals[k] + lax.dot_general(
                    factors[k], mixed, (((0,), (0,)), ((), ())), preferred_element_type=jnp.float32
                )
        for k in range(slots):
            scaled = totals[k] * norm_factor
            turned = scaled.T
            if k == 0:
                scaled = scaled + turned
            for s in range(chunks):
                rows_ref[s, 0, k] = scaled[s * part : (s + 1) * part]
                if k > 0:
                    turned_ref[s, 0, k - 1] = turned[s * part : (s + 1) * part].astype(jnp.bfloat16)

    return pl.pallas_call(
        body,
        out_shape=(
            jax.ShapeDtypeStruct((chunks, per_group, slots, part, width), jnp.float32),
            jax.ShapeDtypeStruct((chunks, per_group, levels, part, width), jnp.bfloat16),
        ),
        grid_spec=pltpu.PrefetchScalarGridSpec(
            num_scalar_prefetch=1,
            grid=(per_group,),
            in_specs=[
                pl.BlockSpec((chunks, 1, rows, width), lambda t, g: (0, t, 0, 0)),
                pl.BlockSpec((chunks, levels, 1, rows, width), lambda t, g: (0, 0, t, 0, 0)),
                pl.BlockSpec((1, slots, width, width), lambda t, g: (g[0] * per_group + t, 0, 0, 0)),
            ],
            out_specs=[
                pl.BlockSpec((chunks, 1, slots, part, width), lambda t, g: (0, t, 0, 0, 0)),
                pl.BlockSpec((chunks, 1, levels, part, width), lambda t, g: (0, t, 0, 0, 0)),
            ],
        ),
        name="gradient_terms",
    )(group_index, own, fetched, precision)


def add_turned(slots_of, own_rows, incoming):
    count, slots, part, width = own_rows.shape
    levels = slots - 1

    def body(index_ref, rows_ref, *refs):
        out_ref = refs[levels]
        out_ref[0, 0] = rows_ref[0, 0]
        for k in range(levels):
            out_ref[0, k + 1] = rows_ref[0, k + 1] + refs[k][0].astype(jnp.float32)

    def source(k):
        return pl.BlockSpec((1, part, width), lambda t, index: (index[t * levels + k], 0, 0))

    return pl.pallas_call(
        body,
        out_shape=jax.ShapeDtypeStruct(own_rows.shape, jnp.float32),
        grid_spec=pltpu.PrefetchScalarGridSpec(
            num_scalar_prefetch=1,
            grid=(count,),
            in_specs=[pl.BlockSpec((1, slots, part, width), lambda t, index: (t, 0, 0, 0))]
            + [source(k) for k in range(levels)],
            out_specs=pl.BlockSpec((1, slots, part, width), lambda t, index: (t, 0, 0, 0)),
        ),
        name="add_turned",
    )(slots_of, own_rows, *([incoming] * levels))


def shards(samples, precision_blocks, pair_rows):
    peers = lax.axis_size("var")
    chunks = lax.axis_size("samp")
    rows = samples.shape[0]
    count, slots, width, _ = precision_blocks.shape
    levels = slots - 1
    per_group = count // chunks
    entries = levels * count
    part = width // chunks
    norm_factor = 0.5 / (rows * chunks)

    partners = pair_rows[:, 1:] // count
    owner = partners.reshape(entries)
    entry_ids = lax.iota(jnp.int32, entries)
    hit = owner[None, :] == lax.iota(jnp.int32, peers)[:, None]
    entry_to = jnp.sum(jnp.where(hit, entry_ids[None, :], 0), axis=1).astype(jnp.int32)

    everything = lax.iota(jnp.int32, count)
    own = pick_columns(everything, samples, width, 4)
    own = lax.all_to_all(own, "samp", 0, 0, tiled=True)
    own = own.reshape(chunks, per_group, rows, width)

    outgoing = pick_columns(entry_to // levels, samples, width, 8)
    incoming = lax.all_to_all(outgoing, "var", 0, 0, tiled=True)
    by_group = jnp.transpose(partners.reshape(chunks, per_group, levels), (0, 2, 1)).reshape(entries)
    fetched = pick_blocks(by_group, incoming, 4)
    fetched = lax.all_to_all(fetched, "samp", 0, 0, tiled=True)
    fetched = fetched.reshape(chunks, levels, per_group, rows, width)

    group_index = lax.axis_index("samp").astype(jnp.int32).reshape(1)
    own_rows, turned = gradient_terms(group_index, own, fetched, precision_blocks, norm_factor)

    turned = lax.all_to_all(turned.reshape(chunks * per_group * levels, part, width), "samp", 0, 0, tiled=True)
    own_rows = lax.all_to_all(own_rows.reshape(count, slots, part, width), "samp", 0, 0, tiled=True)
    sent = pick_blocks(entry_to, turned, 8)
    received = lax.all_to_all(sent, "var", 0, 0, tiled=True)
    return add_turned(owner, own_rows, received)


def solution(mesh):
    placed = (P("samp", "var"), P("var", None, None, None), P("var", None))
    return jax.shard_map(
        shards, mesh=mesh, in_specs=placed, out_specs=P("var", None, "samp", None), check_vma=False
    )
```

```python
import functools

import jax
import jax.numpy as jnp
import numpy as np
from jax import lax
from jax.experimental import pallas as pl
from jax.experimental.pallas import tpu as pltpu
from jax.sharding import PartitionSpec as P

DIMS = (4, 8, 2)
CHUNK = 4
LADDER = ((16, 11, 7, 2), (16, 12, 8, 3), (17, 13, 8, 3), (18, 14, 9, 3), (19, 15, 10, 4), (22, 17, 12, 4))
MESH = pl.DeviceIdType.MESH


def ring_limits():
    group = DIMS[0] * DIMS[2]
    half = DIMS[1] // 2
    return tuple(group * (half - h) + (group + 1) // 2 for h in range(1, half + 1))


def ladder():
    limits = ring_limits()
    steps = [tuple(min(a, b) for a, b in zip(step, limits)) for step in LADDER if len(step) == len(limits)]
    return tuple(steps) + (limits,)


def pick_blocks(picked, blocks, group):
    _, rows, width = blocks.shape
    count = picked.shape[0]
    group = min(group, count)

    def body(index_ref, *refs):
        for i in range(group):
            refs[group][i] = refs[i][0]

    def source(i):
        return pl.BlockSpec((1, rows, width), lambda g, index: (index[g * group + i], 0, 0))

    return pl.pallas_call(
        body,
        out_shape=jax.ShapeDtypeStruct((count, rows, width), blocks.dtype),
        grid_spec=pltpu.PrefetchScalarGridSpec(
            num_scalar_prefetch=1,
            grid=(count // group,),
            in_specs=[source(i) for i in range(group)],
            out_specs=pl.BlockSpec((group, rows, width), lambda g, index: (g, 0, 0)),
        ),
        name="pick_blocks",
    )(picked, *([blocks] * group))


def gradient_terms(group_index, own, fetched, precision, norm_factor):
    chunks, levels, per_group, rows, width = fetched.shape
    slots = levels + 1
    part = width // chunks

    def body(index_ref, own_ref, fetched_ref, p_ref, rows_ref, turned_ref):
        totals = [jnp.zeros((width, width), jnp.float32) for _ in range(slots)]
        for s in range(chunks):
            factors = [own_ref[s]] + [fetched_ref[s, k, 0] for k in range(levels)]
            mixed = jnp.zeros((rows, width), jnp.float32)
            for k in range(slots):
                mixed = mixed + jnp.dot(factors[k], p_ref[0, k], preferred_element_type=jnp.float32)
            mixed = mixed.astype(jnp.bfloat16)
            for k in range(slots):
                totals[k] = totals[k] + lax.dot_general(
                    factors[k], mixed, (((0,), (0,)), ((), ())), preferred_element_type=jnp.float32
                )
        for k in range(slots):
            scaled = totals[k] * norm_factor
            turned = scaled.T
            if k == 0:
                scaled = scaled + turned
            for s in range(chunks):
                rows_ref[s, 0, k] = scaled[s * part : (s + 1) * part]
                if k > 0:
                    turned_ref[s, 0, k - 1] = turned[s * part : (s + 1) * part].astype(jnp.bfloat16)

    return pl.pallas_call(
        body,
        out_shape=(
            jax.ShapeDtypeStruct((chunks, per_group, slots, part, width), jnp.float32),
            jax.ShapeDtypeStruct((chunks, per_group, levels, part, width), jnp.bfloat16),
        ),
        grid_spec=pltpu.PrefetchScalarGridSpec(
            num_scalar_prefetch=1,
            grid=(per_group,),
            in_specs=[
                pl.BlockSpec((chunks, rows, width), lambda t, g: (0, 0, t)),
                pl.BlockSpec((chunks, levels, 1, rows, width), lambda t, g: (0, 0, t, 0, 0)),
                pl.BlockSpec((1, slots, width, width), lambda t, g: (g[0] * per_group + t, 0, 0, 0)),
            ],
            out_specs=[
                pl.BlockSpec((chunks, 1, slots, part, width), lambda t, g: (0, t, 0, 0, 0)),
                pl.BlockSpec((chunks, 1, levels, part, width), lambda t, g: (0, t, 0, 0, 0)),
            ],
        ),
        name="gradient_terms",
    )(group_index, own, fetched, precision)


def add_turned(slots_of, own_rows, incoming):
    count, slots, part, width = own_rows.shape
    levels = slots - 1

    def body(index_ref, rows_ref, *refs):
        out_ref = refs[levels]
        out_ref[0, 0] = rows_ref[0, 0]
        for k in range(levels):
            out_ref[0, k + 1] = rows_ref[0, k + 1] + refs[k][0].astype(jnp.float32)

    def source(k):
        return pl.BlockSpec((1, part, width), lambda t, index: (index[t * levels + k], 0, 0))

    return pl.pallas_call(
        body,
        out_shape=jax.ShapeDtypeStruct(own_rows.shape, jnp.float32),
        grid_spec=pltpu.PrefetchScalarGridSpec(
            num_scalar_prefetch=1,
            grid=(count,),
            in_specs=[pl.BlockSpec((1, slots, part, width), lambda t, index: (t, 0, 0, 0))]
            + [source(k) for k in range(levels)],
            out_specs=pl.BlockSpec((1, slots, part, width), lambda t, index: (t, 0, 0, 0)),
        ),
        name="add_turned",
    )(slots_of, own_rows, *([incoming] * levels))


def route_tables(pair_rows, peers):
    x_size, z_size, cores = DIMS
    count, slots = pair_rows.shape
    levels = slots - 1
    entries = count * levels
    limits = ring_limits()
    half = z_size // 2
    me = lax.axis_index("var").astype(jnp.int32)
    x, z, core = me // (z_size * cores), (me // cores) % z_size, me % cores
    owner = (pair_rows[:, 1:] // count).reshape(entries)
    px, pz, pcore = owner // (z_size * cores), (owner // cores) % z_size, owner % cores
    cx, cz, cc = jnp.bitwise_xor(px, x), jnp.bitwise_xor(pz, z), jnp.bitwise_xor(pcore, core)
    e_ids = lax.iota(jnp.int32, entries)
    column = e_ids // levels
    earlier = e_ids[None, :] < e_ids[:, None]

    same_cz = cz[None, :] == cz[:, None]
    rank = jnp.sum(jnp.where(same_cz & earlier, 1, 0), axis=1)
    zs = lax.iota(jnp.int32, z_size)[:, None]
    right = (jnp.bitwise_xor(zs, cz[None, :]) - zs) % z_size
    goes_right = (right < half) | ((right == half) & (rank % 2 == 0)[None, :])
    hops = jnp.where(goes_right, right, z_size - right)
    side = jnp.where(right == 0, 2, jnp.where(goes_right, 0, 1))
    order = hops * entries - e_ids[None, :]
    ahead = (side[:, :, None] == side[:, None, :]) & (order[:, None, :] > order[:, :, None])
    place = jnp.sum(jnp.where(ahead, 1, 0), axis=2)

    depth = lax.iota(jnp.int32, half) + 1
    load = [
        jnp.max(jnp.sum(jnp.where((side == s)[:, :, None] & (hops[:, :, None] >= depth), 1, 0), axis=1), axis=0)
        for s in (0, 1)
    ]
    load = jnp.maximum(load[0], load[1])
    steps = jnp.asarray(np.array(ladder(), np.int32))
    fits = jnp.all(steps >= load[None, :], axis=1)
    rung = jnp.min(jnp.where(fits, lax.iota(jnp.int32, steps.shape[0]), steps.shape[0] - 1))

    def at(table, z_of):
        return jnp.sum(jnp.where(zs == z_of[None, :], table, 0), axis=0)

    z_all = jnp.full((entries,), z)
    my_side, my_place = at(side, z_all), at(place, z_all)
    gathered = (((px - x) % x_size) * cores + cc) * count + column
    length = limits[0]
    spots = lax.iota(jnp.int32, 2 * length + max(x_size * cores, 1))
    spot = jnp.where(my_side == 2, 2 * length + my_place, my_side * length + my_place)
    taken = spots[:, None] == spot[None, :]
    list_column = jnp.sum(jnp.where(taken, column[None, :], 0), axis=1)
    list_gathered = jnp.sum(jnp.where(taken, gathered[None, :], 0), axis=1)

    offsets = [0]
    for limit in limits:
        offsets.append(offsets[-1] + limit)
    from_side, from_place, from_hops = at(side, pz), at(place, pz), at(hops, pz)
    start = jnp.zeros((entries,), jnp.int32)
    for h in range(1, half + 1):
        start = jnp.where(from_hops == h, offsets[h - 1], start)
    landed = from_side * offsets[-1] + start + from_place
    landed_first = jnp.where(cz == 0, 2 * offsets[-1] + column, landed)
    landed_second = jnp.where(cz == 0, 2 * offsets[-1] + my_place, landed)
    slot = (cx * cores + cc) * z_size + cz
    slot_source = jnp.sum(
        jnp.where(lax.iota(jnp.int32, peers)[:, None] == slot[None, :], landed_first[None, :], 0), axis=1
    )
    table = jnp.concatenate([list_column, list_gathered, slot_source, slot, landed_second]).astype(jnp.int32)
    return rung, table, owner, e_ids


def exchange_body(steps, collective, table_ref, x_ref, own_ref, fetched_ref, list_first, list_second, ring_first,
                  ring_second, own_first, gathered, slots_out, slots_in, passing, stage, local_sem, send_sem, recv_sem):
    x_size, z_size, cores = DIMS
    chunks = lax.axis_size("samp")
    rows, total = x_ref.shape
    width = fetched_ref.shape[-1]
    count = total // width
    levels = fetched_ref.shape[1]
    per_group = fetched_ref.shape[2]
    entries = count * levels
    half_rows = rows // 2
    half = z_size // 2
    limits = ring_limits()
    length = limits[0]
    offsets = [0]
    for limit in limits:
        offsets.append(offsets[-1] + limit)
    local = x_size * cores
    base_gathered = 2 * length + local
    base_source = 2 * base_gathered
    base_slot = base_source + x_size * z_size * cores
    base_landed = base_slot + entries

    me = lax.axis_index("var")
    group = lax.axis_index("samp")
    x, z, core = me // (z_size * cores), (me // cores) % z_size, me % cores

    def device(dx=0, dz=0, dc=0):
        return (group, (((x + dx) % x_size) * z_size + (z + dz) % z_size) * cores + (core + dc) % cores)

    def plane(dy):
        return ((group + dy) % chunks, me)

    copies = []

    def remote(src, dst, target):
        index = len(copies)
        copy = pltpu.make_async_remote_copy(
            src_ref=src, dst_ref=dst, send_sem=send_sem.at[index], recv_sem=recv_sem.at[index],
            device_id=target, device_id_type=MESH,
        )
        copies.append(copy)
        copy.start()
        return copy

    barrier = pltpu.get_barrier_semaphore()
    friends = [device(dz=1), device(dz=-1)]
    if x_size > 1:
        friends += [device(dx=dx, dc=dc) for dx in (1, -1) for dc in range(cores)]
    friends += [device(dc=dc) for dc in range(1, cores)]
    friends += [plane(dy) for dy in range(1, chunks)]
    for friend in friends:
        pl.semaphore_signal(barrier, inc=1, device_id=friend, device_id_type=MESH)
    pl.semaphore_wait(barrier, len(friends))

    def column_of(index):
        return pl.ds(pl.multiple_of(index * width, width), width)

    def ranges(limit):
        return [(a, min(a + CHUNK, limit)) for a in range(0, limit, CHUNK)]

    def first_hop(lists, ring, fill):
        sent = {}
        for j, (a, b) in enumerate(ranges(steps[0])):
            for s, dz in ((0, 1), (1, -1)):
                @pl.loop(a, b)
                def _(p):
                    fill(s, p)
                sent[j, s] = remote(lists.at[s, pl.ds(a, b - a)], ring.at[pl.ds(s * offsets[-1] + a, b - a)], device(dz=dz))
        return sent

    def next_hop(h, before, ring):
        sent = {}
        for j, (a, b) in enumerate(ranges(steps[h])):
            for s, dz in ((0, 1), (1, -1)):
                before[j, s].wait_recv()
                at = s * offsets[-1]
                sent[j, s] = remote(
                    ring.at[pl.ds(at + offsets[h - 1] + a, b - a)], ring.at[pl.ds(at + offsets[h] + a, b - a)], device(dz=dz)
                )
        return sent

    @pl.loop(0, count)
    def _(t):
        own_first[t] = x_ref[0:half_rows, column_of(t)]
        gathered[t] = x_ref[half_rows:rows, column_of(t)]

    def fill_first(s, p):
        list_first[s, p] = own_first[table_ref[s * length + p]]

    hop = first_hop(list_first, ring_first, fill_first)
    def slab(dx, dc, first=0, size=count):
        return gathered.at[pl.ds((dx * cores + dc) * count + first, size)]

    slabs = []
    if x_size > 1:
        to_right = remote(slab(0, 0), slab(x_size - 1, 0), device(dx=1))
        to_left = remote(slab(0, 0), slab(1, 0), device(dx=-1))
    if cores > 1:
        slabs.append(remote(slab(0, 0), slab(0, 1), device(dc=1)))
    wide = total // chunks

    def quarter(which):
        return pl.ds(pl.multiple_of(which * wide, width), wide)

    own_copies = [
        remote(x_ref.at[:, quarter((group + dy) % chunks)], own_ref.at[group], plane(dy)) for dy in range(1, chunks)
    ]
    own_keep = pltpu.make_async_copy(x_ref.at[:, quarter(group)], own_ref.at[group], local_sem.at[0])
    own_keep.start()

    @pl.loop(0, count)
    def _(t):
        ring_first[2 * offsets[-1] + t] = x_ref[0:half_rows, column_of(t)]

    def share(dx):
        if cores > 1:
            slabs.append(remote(slab(dx, 0), slab(dx, 1), device(dc=1)))

    far = []
    for h in range(1, half):
        later = next_hop(h, hop, ring_first)
        for (j, s), copy in hop.items():
            if (j, s) not in later:
                copy.wait_recv()
        hop = later
        if h == 1 and x_size > 1:
            to_right.wait_recv()
            to_left.wait_recv()
            some = count // 2
            far = [
                remote(slab(x_size - 1, 0, 0, some), slab(2, 0, 0, some), device(dx=1)),
                remote(slab(1, 0, some, some), slab(2, 0, some, some), device(dx=-1)),
            ]
            share(1)
            share(x_size - 1)
        if h == 2 or half <= 2:
            for copy in far:
                copy.wait_recv()
            if far:
                share(2)
            far = []
    for copy in slabs:
        copy.wait_recv()

    def fill_second(s, p):
        list_second[s, p] = gathered[table_ref[base_gathered + s * length + p]]

    last = hop
    hop = first_hop(list_second, ring_second, fill_second)

    @pl.loop(0, local)
    def _(p):
        ring_second[2 * offsets[-1] + p] = gathered[table_ref[base_gathered + 2 * length + p]]

    for copy in last.values():
        copy.wait_recv()

    def fill_slots(which):
        @pl.loop(which * z_size, (which + 1) * z_size)
        def _(p):
            slots_out[p] = ring_first[table_ref[base_source + p]]
        return pl.ds(which * z_size, z_size)

    across, relays = [], []
    if x_size > 1:
        relays = [
            remote(slots_out.at[fill_slots(2 * cores + dc)], passing.at[dc], device(dx=(1, -1)[dc])) for dc in range(cores)
        ]
        odd = x % 2
        for dc in range(cores):
            part = fill_slots(cores + dc)
            across.append(remote(slots_out.at[part], slots_in.at[part], device(dx=1 - 2 * odd, dc=dc)))
            part = fill_slots(3 * cores + dc)
            across.append(remote(slots_out.at[part], slots_in.at[part], device(dx=2 * odd - 1, dc=dc)))
    if cores > 1:
        part = fill_slots(1)
        across.append(remote(slots_out.at[part], slots_in.at[part], device(dc=1)))

    @pl.loop(0, z_size)
    def _(p):
        slots_in[p] = ring_first[table_ref[base_source + p]]

    def stage_entries(row, load):
        for k in range(levels):
            @pl.loop(0, count)
            def _(t):
                stage[t // per_group, k * per_group + t % per_group, pl.ds(row, half_rows)] = load(t * levels + k)

    def to_planes(row):
        for dy in range(1, chunks):
            target = (group + dy) % chunks
            part = pl.ds(row, half_rows)
            for k in range(levels):
                arriving.append(
                    remote(stage.at[target, pl.ds(k * per_group, per_group), part], fetched_ref.at[group, k, :, part], plane(dy))
                )
        kept = []
        for k in range(levels):
            copy = pltpu.make_async_copy(
                stage.at[group, pl.ds(k * per_group, per_group), pl.ds(row, half_rows)],
                fetched_ref.at[group, k, :, pl.ds(row, half_rows)],
                local_sem.at[1 + (levels if row else 0) + k],
            )
            copy.start()
            kept.append(copy)
        return kept

    arriving, kept = [], []

    def finish_first():
        for copy in across:
            copy.wait_recv()
        stage_entries(0, lambda e: slots_in[table_ref[base_slot + e]])
        kept.extend(to_planes(0))

    for h in range(1, half):
        later = next_hop(h, hop, ring_second)
        for (j, s), copy in hop.items():
            if (j, s) not in later:
                copy.wait_recv()
        hop = later
        if h == 1:
            for dc, copy in enumerate(relays):
                copy.wait_recv()
                part = pl.ds((2 * cores + dc) * z_size, z_size)
                across.append(remote(passing.at[dc], slots_in.at[part], device(dx=(1, -1)[dc], dc=dc)))
        if h == 2:
            finish_first()
    if half <= 2:
        finish_first()
    for copy in hop.values():
        copy.wait_recv()
    stage_entries(half_rows, lambda e: ring_second[table_ref[base_landed + e]])
    kept.extend(to_planes(half_rows))

    for copy in arriving + own_copies:
        copy.wait_recv()
    for copy in kept + [own_keep]:
        copy.wait()
    for copy in copies:
        copy.wait_send()


def exchange(steps, collective, table, samples, levels, width, chunks):
    x_size, z_size, cores = DIMS
    rows, total = samples.shape
    count = total // width
    per_group = count // chunks
    half_rows = rows // 2
    limits = ring_limits()
    landing = 2 * sum(limits)
    block = (half_rows, width)
    copies = 160
    scratch = [
        pltpu.VMEM((2, limits[0], *block), jnp.bfloat16),
        pltpu.VMEM((2, limits[0], *block), jnp.bfloat16),
        pltpu.VMEM((landing + count, *block), jnp.bfloat16),
        pltpu.VMEM((landing + x_size * cores, *block), jnp.bfloat16),
        pltpu.VMEM((count, *block), jnp.bfloat16),
        pltpu.VMEM((x_size * cores * count, *block), jnp.bfloat16),
        pltpu.VMEM((x_size * cores * z_size, *block), jnp.bfloat16),
        pltpu.VMEM((x_size * cores * z_size, *block), jnp.bfloat16),
        pltpu.VMEM((cores, z_size, *block), jnp.bfloat16),
        pltpu.VMEM((chunks, levels * per_group, rows, width), jnp.bfloat16),
        pltpu.SemaphoreType.DMA((1 + 2 * levels,)),
        pltpu.SemaphoreType.DMA((copies,)),
        pltpu.SemaphoreType.DMA((copies,)),
    ]
    return pl.pallas_call(
        functools.partial(exchange_body, steps, collective),
        out_shape=(
            jax.ShapeDtypeStruct((chunks, rows, total // chunks), jnp.bfloat16),
            jax.ShapeDtypeStruct((chunks, levels, per_group, rows, width), jnp.bfloat16),
        ),
        in_specs=[pl.BlockSpec(memory_space=pltpu.SMEM), pl.BlockSpec(memory_space=pltpu.VMEM)],
        out_specs=[pl.BlockSpec(memory_space=pl.ANY)] * 2,
        scratch_shapes=scratch,
        compiler_params=pltpu.CompilerParams(
            collective_id=collective, has_side_effects=True, vmem_limit_bytes=60 * 2**20
        ),
        name=f"exchange_{collective}",
    )(table, samples)


def shards(samples, precision_blocks, pair_rows):
    peers = lax.axis_size("var")
    chunks = lax.axis_size("samp")
    rows = samples.shape[0]
    count, slots, width, _ = precision_blocks.shape
    levels = slots - 1
    per_group = count // chunks
    part = width // chunks
    norm_factor = 0.5 / (rows * chunks)

    rung, table, owner, entry_ids = route_tables(pair_rows, peers)
    hit = owner[None, :] == lax.iota(jnp.int32, peers)[:, None]
    entry_to = jnp.sum(jnp.where(hit, entry_ids[None, :], 0), axis=1).astype(jnp.int32)

    branches = [
        functools.partial(exchange, steps, i, levels=levels, width=width, chunks=chunks)
        for i, steps in enumerate(ladder())
    ]
    own, fetched = lax.switch(rung, branches, table, samples)

    group_index = lax.axis_index("samp").astype(jnp.int32).reshape(1)
    own_rows, turned = gradient_terms(group_index, own, fetched, precision_blocks, norm_factor)

    turned = lax.all_to_all(turned.reshape(chunks * per_group * levels, part, width), "samp", 0, 0, tiled=True)
    own_rows = lax.all_to_all(own_rows.reshape(count, slots, part, width), "samp", 0, 0, tiled=True)
    sent = pick_blocks(entry_to, turned, 8)
    received = lax.all_to_all(sent, "var", 0, 0, tiled=True)
    return add_turned(owner, own_rows, received)


def solution(mesh):
    placed = (P("samp", "var"), P("var", None, None, None), P("var", None))
    return jax.shard_map(
        shards, mesh=mesh, in_specs=placed, out_specs=P("var", None, "samp", None), check_vma=False
    )
```

```python
import functools

import jax
import jax.numpy as jnp
import numpy as np
from jax import lax
from jax.experimental import pallas as pl
from jax.experimental.pallas import tpu as pltpu
from jax.sharding import PartitionSpec as P

DIMS = (4, 8, 2)
CHUNK = 4
LADDER = ((16, 12, 8, 3), (17, 13, 8, 3), (18, 14, 9, 3), (20, 16, 11, 4))
SWAP_LADDER = ((16, 12, 8, 3), (18, 14, 9, 3), (20, 16, 11, 4))
MESH = pl.DeviceIdType.MESH


def ring_limits():
    group = DIMS[0] * DIMS[2]
    half = DIMS[1] // 2
    return tuple(group * (half - h) + (group + 1) // 2 for h in range(1, half + 1))


def offsets_of(limits):
    offsets = [0]
    for limit in limits:
        offsets.append(offsets[-1] + limit)
    return offsets


def ladder(rungs):
    limits = ring_limits()
    steps = [tuple(min(a, b) for a, b in zip(step, limits)) for step in rungs if len(step) == len(limits)]
    return tuple(steps) + (limits,)


def gradient_terms(group_index, own, fetched, precision, norm_factor):
    chunks, levels, per_group, rows, width = fetched.shape
    slots = levels + 1
    part = width // chunks

    def body(index_ref, own_ref, fetched_ref, p_ref, rows_ref, turned_ref):
        totals = [jnp.zeros((width, width), jnp.float32) for _ in range(slots)]
        for s in range(chunks):
            factors = [own_ref[s]] + [fetched_ref[s, k, 0] for k in range(levels)]
            mixed = jnp.zeros((rows, width), jnp.float32)
            for k in range(slots):
                mixed = mixed + jnp.dot(factors[k], p_ref[0, k], preferred_element_type=jnp.float32)
            mixed = mixed.astype(jnp.bfloat16)
            for k in range(slots):
                totals[k] = totals[k] + lax.dot_general(
                    factors[k], mixed, (((0,), (0,)), ((), ())), preferred_element_type=jnp.float32
                )
        for k in range(slots):
            scaled = totals[k] * norm_factor
            turned = scaled.T
            if k == 0:
                scaled = scaled + turned
            for s in range(chunks):
                rows_ref[s, 0, k] = scaled[s * part : (s + 1) * part]
                if k > 0:
                    turned_ref[s, 0, k - 1] = turned[s * part : (s + 1) * part].astype(jnp.bfloat16)

    return pl.pallas_call(
        body,
        out_shape=(
            jax.ShapeDtypeStruct((chunks, per_group, slots, part, width), jnp.float32),
            jax.ShapeDtypeStruct((chunks, per_group, levels, part, width), jnp.bfloat16),
        ),
        grid_spec=pltpu.PrefetchScalarGridSpec(
            num_scalar_prefetch=1,
            grid=(per_group,),
            in_specs=[
                pl.BlockSpec((chunks, rows, width), lambda t, g: (0, 0, t)),
                pl.BlockSpec((chunks, levels, 1, rows, width), lambda t, g: (0, 0, t, 0, 0)),
                pl.BlockSpec((1, slots, width, width), lambda t, g: (g[0] * per_group + t, 0, 0, 0)),
            ],
            out_specs=[
                pl.BlockSpec((chunks, 1, slots, part, width), lambda t, g: (0, t, 0, 0, 0)),
                pl.BlockSpec((chunks, 1, levels, part, width), lambda t, g: (0, t, 0, 0, 0)),
            ],
        ),
        name="gradient_terms",
    )(group_index, own, fetched, precision)


def add_turned(own_rows, turned):
    count, slots, part, width = own_rows.shape
    levels = slots - 1
    group = min(4, count)

    def body(rows_ref, turned_ref, out_ref):
        for i in range(group):
            out_ref[i, 0] = rows_ref[i, 0]
            for k in range(levels):
                out_ref[i, k + 1] = rows_ref[i, k + 1] + turned_ref[i, k].astype(jnp.float32)

    def blocks(slots):
        return pl.BlockSpec((group, slots, part, width), lambda t: (t, 0, 0, 0))

    return pl.pallas_call(
        body,
        out_shape=jax.ShapeDtypeStruct(own_rows.shape, jnp.float32),
        grid=(count // group,),
        in_specs=[blocks(slots), blocks(levels)],
        out_specs=blocks(slots),
        name="add_turned",
    )(own_rows, turned)


def route_tables(pair_rows, peers):
    x_size, z_size, cores = DIMS
    count, slots = pair_rows.shape
    levels = slots - 1
    entries = count * levels
    limits = ring_limits()
    half = z_size // 2
    me = lax.axis_index("var").astype(jnp.int32)
    x, z, core = me // (z_size * cores), (me // cores) % z_size, me % cores
    owner = (pair_rows[:, 1:] // count).reshape(entries)
    px, pz, pcore = owner // (z_size * cores), (owner // cores) % z_size, owner % cores
    cx, cz, cc = jnp.bitwise_xor(px, x), jnp.bitwise_xor(pz, z), jnp.bitwise_xor(pcore, core)
    e_ids = lax.iota(jnp.int32, entries)
    column = e_ids // levels
    earlier = e_ids[None, :] < e_ids[:, None]

    same_cz = cz[None, :] == cz[:, None]
    rank = jnp.sum(jnp.where(same_cz & earlier, 1, 0), axis=1)
    zs = lax.iota(jnp.int32, z_size)[:, None]
    right = (jnp.bitwise_xor(zs, cz[None, :]) - zs) % z_size
    goes_right = (right < half) | ((right == half) & (rank % 2 == 0)[None, :])
    hops = jnp.where(goes_right, right, z_size - right)
    side = jnp.where(right == 0, 2, jnp.where(goes_right, 0, 1))
    order = hops * entries - e_ids[None, :]
    ahead = (side[:, :, None] == side[:, None, :]) & (order[:, None, :] > order[:, :, None])
    place = jnp.sum(jnp.where(ahead, 1, 0), axis=2)

    depth = lax.iota(jnp.int32, half) + 1
    load = [
        jnp.max(jnp.sum(jnp.where((side == s)[:, :, None] & (hops[:, :, None] >= depth), 1, 0), axis=1), axis=0)
        for s in (0, 1)
    ]
    load = jnp.maximum(load[0], load[1])

    def rung_of(rungs):
        steps = jnp.asarray(np.array(ladder(rungs), np.int32))
        fits = jnp.all(steps >= load[None, :], axis=1)
        return jnp.min(jnp.where(fits, lax.iota(jnp.int32, steps.shape[0]), steps.shape[0] - 1))

    def at(table, z_of):
        return jnp.sum(jnp.where(zs == z_of[None, :], table, 0), axis=0)

    z_all = jnp.full((entries,), z)
    my_side, my_place = at(side, z_all), at(place, z_all)
    gathered = (((px - x) % x_size) * cores + cc) * count + column
    length = limits[0]
    spots = lax.iota(jnp.int32, 2 * length + max(x_size * cores, 1))
    spot = jnp.where(my_side == 2, 2 * length + my_place, my_side * length + my_place)
    taken = spots[:, None] == spot[None, :]
    list_column = jnp.sum(jnp.where(taken, column[None, :], 0), axis=1)
    list_gathered = jnp.sum(jnp.where(taken, gathered[None, :], 0), axis=1)

    offsets = offsets_of(limits)
    from_side, from_place, from_hops = at(side, pz), at(place, pz), at(hops, pz)
    start = jnp.zeros((entries,), jnp.int32)
    for h in range(1, half + 1):
        start = jnp.where(from_hops == h, offsets[h - 1], start)
    landed = from_side * offsets[-1] + start + from_place
    landed_first = jnp.where(cz == 0, 2 * offsets[-1] + column, landed)
    landed_second = jnp.where(cz == 0, 2 * offsets[-1] + my_place, landed)
    slot = (cx * cores + cc) * z_size + cz
    at_slot = lax.iota(jnp.int32, peers)[:, None] == slot[None, :]
    slot_first, slot_second, slot_entry = (
        jnp.sum(jnp.where(at_slot, values[None, :], 0), axis=1) for values in (landed_first, landed_second, e_ids)
    )
    list_entry = jnp.sum(jnp.where(taken, e_ids[None, :], 0), axis=1)
    list_slot = jnp.sum(jnp.where(taken, slot[None, :], 0), axis=1)
    exchange_table = jnp.concatenate([list_column, list_gathered, slot_first, slot, landed_second]).astype(jnp.int32)
    swap_table = jnp.concatenate([list_entry, list_slot, slot_second, slot_entry, slot, landed_second]).astype(jnp.int32)
    return rung_of(LADDER), exchange_table, rung_of(SWAP_LADDER), swap_table


class Links:
    def __init__(self, steps, send_sem, recv_sem):
        self.steps, self.send_sem, self.recv_sem = steps, send_sem, recv_sem
        self.x_size, self.z_size, self.cores = DIMS
        self.chunks = lax.axis_size("samp")
        self.offsets = offsets_of(ring_limits())
        self.me = lax.axis_index("var")
        self.group = lax.axis_index("samp")
        self.x = self.me // (self.z_size * self.cores)
        self.z = (self.me // self.cores) % self.z_size
        self.core = self.me % self.cores
        self.copies = []

    def device(self, dx=0, dz=0, dc=0):
        x, z, core = (self.x + dx) % self.x_size, (self.z + dz) % self.z_size, (self.core + dc) % self.cores
        return (self.group, (x * self.z_size + z) * self.cores + core)

    def plane(self, dy):
        return ((self.group + dy) % self.chunks, self.me)

    def remote(self, src, dst, target):
        index = len(self.copies)
        copy = pltpu.make_async_remote_copy(
            src_ref=src, dst_ref=dst, send_sem=self.send_sem.at[index], recv_sem=self.recv_sem.at[index],
            device_id=target, device_id_type=MESH,
        )
        self.copies.append(copy)
        copy.start()
        return copy

    def greet(self):
        barrier = pltpu.get_barrier_semaphore()
        friends = [self.device(dz=1), self.device(dz=-1)]
        if self.x_size > 1:
            friends += [self.device(dx=dx, dc=dc) for dx in (1, -1) for dc in range(self.cores)]
        friends += [self.device(dc=dc) for dc in range(1, self.cores)]
        friends += [self.plane(dy) for dy in range(1, self.chunks)]
        for friend in friends:
            pl.semaphore_signal(barrier, inc=1, device_id=friend, device_id_type=MESH)
        pl.semaphore_wait(barrier, len(friends))

    def first_hop(self, lists, ring, fill):
        sent = {}
        for j, (a, b) in enumerate(ranges(self.steps[0])):
            for s, dz in ((0, 1), (1, -1)):
                @pl.loop(a, b)
                def _(p):
                    fill(s, p)
                landing = ring.at[pl.ds(s * self.offsets[-1] + a, b - a)]
                sent[j, s] = self.remote(lists.at[s, pl.ds(a, b - a)], landing, self.device(dz=dz))
        return sent

    def next_hop(self, h, before, ring):
        sent = {}
        for j, (a, b) in enumerate(ranges(self.steps[h])):
            for s, dz in ((0, 1), (1, -1)):
                before[j, s].wait_recv()
                here = s * self.offsets[-1] + self.offsets[h - 1] + a
                there = s * self.offsets[-1] + self.offsets[h] + a
                sent[j, s] = self.remote(ring.at[pl.ds(here, b - a)], ring.at[pl.ds(there, b - a)], self.device(dz=dz))
        for key, copy in before.items():
            if key not in sent:
                copy.wait_recv()
        return sent

    def across(self, out, landing, passing, fill):
        z_size, cores = self.z_size, self.cores

        def filled(which):
            @pl.loop(which * z_size, (which + 1) * z_size)
            def _(p):
                out[p] = fill(p)
            return pl.ds(which * z_size, z_size)

        arriving, relays = [], []
        if self.x_size > 1:
            for dc in range(cores):
                part = filled(2 * cores + dc)
                relays.append(self.remote(out.at[part], passing.at[dc], self.device(dx=(1, -1)[dc])))
            odd = self.x % 2
            for dc in range(cores):
                part = filled(cores + dc)
                arriving.append(self.remote(out.at[part], landing.at[part], self.device(dx=1 - 2 * odd, dc=dc)))
                part = filled(3 * cores + dc)
                arriving.append(self.remote(out.at[part], landing.at[part], self.device(dx=2 * odd - 1, dc=dc)))
        if cores > 1:
            part = filled(1)
            arriving.append(self.remote(out.at[part], landing.at[part], self.device(dc=1)))

        @pl.loop(0, z_size)
        def _(p):
            landing[p] = fill(p)

        return arriving, relays

    def relay(self, landing, passing, arriving, relays):
        for dc, copy in enumerate(relays):
            copy.wait_recv()
            part = pl.ds((2 * self.cores + dc) * self.z_size, self.z_size)
            arriving.append(self.remote(passing.at[dc], landing.at[part], self.device(dx=(1, -1)[dc], dc=dc)))

    def planes(self, source, landing, passing, pieces):
        arriving, relays = [], []
        four = self.chunks == 4 and pieces == 2
        for dy in range(1, self.chunks):
            target = (self.group + dy) % self.chunks
            if four and dy == 2:
                continue
            for i in range(pieces):
                arriving.append(self.remote(source(target, i), landing(self.group, i), self.plane(dy)))
        if four:
            target = (self.group + 2) % self.chunks
            relays = [
                self.remote(source(target, i), passing(i), self.plane((1, -1)[i])) for i in range(pieces)
            ]

        def pass_on():
            for i, copy in enumerate(relays):
                copy.wait_recv()
                sender = (self.group + (-1, 1)[i]) % self.chunks
                arriving.append(self.remote(passing(i), landing(sender, i), self.plane((1, -1)[i])))

        return arriving, pass_on

    def finish(self, arriving, kept):
        for copy in arriving:
            copy.wait_recv()
        for copy in kept:
            copy.wait()
        for copy in self.copies:
            copy.wait_send()


def ranges(limit):
    return [(a, min(a + CHUNK, limit)) for a in range(0, limit, CHUNK)]


def exchange_body(steps, first_rows, table_ref, x_ref, own_ref, fetched_ref, list_first, list_second, ring_first,
                  ring_second, own_first, gathered, slots_out, slots_in, passing, stage, passing_first, passing_second,
                  local_sem, send_sem, recv_sem):
    links = Links(steps, send_sem, recv_sem)
    x_size, z_size, cores = DIMS
    chunks = links.chunks
    rows, total = x_ref.shape
    width = fetched_ref.shape[-1]
    count = total // width
    levels = fetched_ref.shape[1]
    per_group = fetched_ref.shape[2]
    entries = count * levels
    half = z_size // 2
    length = ring_limits()[0]
    tail = 2 * links.offsets[-1]
    local = x_size * cores
    base_gathered = 2 * length + local
    base_source = 2 * base_gathered
    base_slot = base_source + x_size * z_size * cores
    base_landed = base_slot + entries

    links.greet()

    def column_of(index):
        return pl.ds(pl.multiple_of(index * width, width), width)

    @pl.loop(0, count)
    def _(t):
        own_first[t] = x_ref[0:first_rows, column_of(t)]
        gathered[t] = x_ref[first_rows:rows, column_of(t)]

    def fill_first(s, p):
        list_first[s, p] = own_first[table_ref[s * length + p]]

    hop = links.first_hop(list_first, ring_first, fill_first)

    def slab(dx, dc, first=0, size=count):
        return gathered.at[pl.ds((dx * cores + dc) * count + first, size)]

    slabs = []
    if x_size > 1:
        to_right = links.remote(slab(0, 0), slab(x_size - 1, 0), links.device(dx=1))
        to_left = links.remote(slab(0, 0), slab(1, 0), links.device(dx=-1))
    if cores > 1:
        slabs.append(links.remote(slab(0, 0), slab(0, 1), links.device(dc=1)))

    wide = total // chunks

    def quarter(which):
        return x_ref.at[:, pl.ds(pl.multiple_of(which * wide, width), wide)]

    arriving = [
        links.remote(quarter((links.group + dy) % chunks), own_ref.at[links.group], links.plane(dy))
        for dy in range(1, chunks)
    ]
    kept = [pltpu.make_async_copy(quarter(links.group), own_ref.at[links.group], local_sem.at[0])]
    kept[0].start()

    @pl.loop(0, count)
    def _(t):
        ring_first[tail + t] = own_first[t]

    def share(dx):
        if cores > 1:
            slabs.append(links.remote(slab(dx, 0), slab(dx, 1), links.device(dc=1)))

    far = []
    for h in range(1, half):
        hop = links.next_hop(h, hop, ring_first)
        if h == 1 and x_size > 1:
            to_right.wait_recv()
            to_left.wait_recv()
            some = count // 2
            far = [
                links.remote(slab(x_size - 1, 0, 0, some), slab(2, 0, 0, some), links.device(dx=1)),
                links.remote(slab(1, 0, some, some), slab(2, 0, some, some), links.device(dx=-1)),
            ]
            share(1)
            share(x_size - 1)
        if h == 2 or half <= 2:
            for copy in far:
                copy.wait_recv()
            if far:
                share(2)
            far = []
    for copy in slabs:
        copy.wait_recv()

    def fill_second(s, p):
        list_second[s, p] = gathered[table_ref[base_gathered + s * length + p]]

    last = hop
    hop = links.first_hop(list_second, ring_second, fill_second)

    @pl.loop(0, local)
    def _(p):
        ring_second[tail + p] = gathered[table_ref[base_gathered + 2 * length + p]]

    for copy in last.values():
        copy.wait_recv()
    moved, relays = links.across(slots_out, slots_in, passing, lambda p: ring_first[table_ref[base_source + p]])

    def stage_entries(part, load):
        for k in range(levels):
            @pl.loop(0, count)
            def _(t):
                stage[t // per_group, k * per_group + t % per_group, part] = load(t * levels + k)

    def to_planes(part, relay, sems):
        landed, pass_on = links.planes(
            lambda target, k: stage.at[target, pl.ds(k * per_group, per_group), part],
            lambda sender, k: fetched_ref.at[sender, k, :, part],
            lambda k: relay.at[k],
            levels,
        )
        for k in range(levels):
            copy = pltpu.make_async_copy(
                stage.at[links.group, pl.ds(k * per_group, per_group), part],
                fetched_ref.at[links.group, k, :, part],
                local_sem.at[sems + k],
            )
            copy.start()
            kept.append(copy)
        return landed, pass_on

    def send_first():
        for copy in moved:
            copy.wait_recv()
        part = pl.ds(0, first_rows)
        stage_entries(part, lambda e: slots_in[table_ref[base_slot + e]])
        return to_planes(part, passing_first, 1)

    landed_first = None
    for h in range(1, half):
        hop = links.next_hop(h, hop, ring_second)
        if h == 1:
            links.relay(slots_in, passing, moved, relays)
        if h == 2:
            landed_first, pass_first = send_first()
    if half <= 2:
        landed_first, pass_first = send_first()
    for copy in hop.values():
        copy.wait_recv()
    part = pl.ds(first_rows, rows - first_rows)
    pass_first()
    stage_entries(part, lambda e: ring_second[table_ref[base_landed + e]])
    landed_second, pass_second = to_planes(part, passing_second, 1 + levels)
    pass_second()
    links.finish(arriving + landed_first + landed_second, kept)


def exchange(steps, collective, table, samples, levels, width, chunks):
    x_size, z_size, cores = DIMS
    rows, total = samples.shape
    count = total // width
    per_group = count // chunks
    first_rows = rows * 3 // 8 if rows % 128 == 0 else rows // 2
    limits = ring_limits()
    landing = 2 * sum(limits)
    first, second = (first_rows, width), (rows - first_rows, width)
    peers = x_size * z_size * cores
    copies = 160

    def space(*shape):
        return pltpu.VMEM(shape, jnp.bfloat16)

    scratch = [
        space(2, limits[0], *first),
        space(2, limits[0], *second),
        space(landing + count, *first),
        space(landing + x_size * cores, *second),
        space(count, *first),
        space(x_size * cores * count, *second),
        space(peers, *first),
        space(peers, *first),
        space(cores, z_size, *first),
        space(chunks, levels * per_group, rows, width),
        space(levels, per_group, *first),
        space(levels, per_group, *second),
        pltpu.SemaphoreType.DMA((1 + 2 * levels,)),
        pltpu.SemaphoreType.DMA((copies,)),
        pltpu.SemaphoreType.DMA((copies,)),
    ]
    return pl.pallas_call(
        functools.partial(exchange_body, steps, first_rows),
        out_shape=(
            jax.ShapeDtypeStruct((chunks, rows, total // chunks), jnp.bfloat16),
            jax.ShapeDtypeStruct((chunks, levels, per_group, rows, width), jnp.bfloat16),
        ),
        in_specs=[pl.BlockSpec(memory_space=pltpu.SMEM), pl.BlockSpec(memory_space=pltpu.VMEM)],
        out_specs=[pl.BlockSpec(memory_space=pl.ANY)] * 2,
        scratch_shapes=scratch,
        compiler_params=pltpu.CompilerParams(
            collective_id=collective, has_side_effects=True, vmem_limit_bytes=61 * 2**20
        ),
        name=f"exchange_{collective}",
    )(table, samples)


def swap_body(steps, table_ref, rows_ref, turned_ref, out_rows_ref, got_ref, mine, list_first, list_second, ring_first,
              ring_second, out_first, in_first, out_second, in_second, passing_first, passing_second, passing_turned,
              passing_rows, local_sem, send_sem, recv_sem):
    links = Links(steps, send_sem, recv_sem)
    x_size, z_size, cores = DIMS
    chunks = links.chunks
    per_group = rows_ref.shape[1]
    entries, part, width = got_ref.shape
    each = entries // chunks
    half_part = part // 2
    half = z_size // 2
    length = ring_limits()[0]
    tail = 2 * links.offsets[-1]
    local = x_size * cores
    peers = x_size * z_size * cores
    base_slots = 2 * length + local
    base_source = 2 * base_slots
    base_entry = base_source + peers
    base_slot = base_entry + peers
    base_landed = base_slot + entries
    upper, lower = slice(0, half_part), slice(half_part, part)

    links.greet()
    kept = [
        pltpu.make_async_copy(turned_ref.at[links.group], mine.at[pl.ds(links.group * each, each)], local_sem.at[0]),
        pltpu.make_async_copy(
            rows_ref.at[links.group], out_rows_ref.at[pl.ds(links.group * per_group, per_group)], local_sem.at[1]
        ),
    ]
    for copy in kept:
        copy.start()
    some = each // 2
    arrived, pass_turned = links.planes(
        lambda target, i: turned_ref.at[target, pl.ds(i * some, some)],
        lambda sender, i: mine.at[pl.ds(sender * each + i * some, some)],
        lambda i: passing_turned.at[i],
        2,
    )
    pass_turned()
    few = per_group // 2 if per_group > 1 else 1
    arriving, pass_rows = links.planes(
        lambda target, i: rows_ref.at[target, pl.ds(i * few, few)],
        lambda sender, i: out_rows_ref.at[pl.ds(sender * per_group + i * few, few)],
        lambda i: passing_rows.at[i],
        per_group // few,
    )
    for copy in arrived:
        copy.wait_recv()
    kept[0].wait()

    def fill_first(s, p):
        list_first[s, p] = mine[table_ref[s * length + p], upper]

    hop = links.first_hop(list_first, ring_first, fill_first)
    moved, relays = links.across(
        out_second, in_second, passing_second, lambda p: mine[table_ref[base_entry + p], lower]
    )

    @pl.loop(0, local)
    def _(p):
        ring_first[tail + p] = mine[table_ref[2 * length + p], upper]

    for h in range(1, half):
        hop = links.next_hop(h, hop, ring_first)
        if h == 1:
            links.relay(in_second, passing_second, moved, relays)
    if half == 1:
        links.relay(in_second, passing_second, moved, relays)
    for copy in moved:
        copy.wait_recv()

    def fill_second(s, p):
        list_second[s, p] = in_second[table_ref[base_slots + s * length + p]]

    last = hop
    hop = links.first_hop(list_second, ring_second, fill_second)

    @pl.loop(0, local)
    def _(p):
        ring_second[tail + p] = in_second[table_ref[base_slots + 2 * length + p]]

    for copy in last.values():
        copy.wait_recv()
    moved, relays = links.across(
        out_first, in_first, passing_first, lambda p: ring_first[table_ref[base_source + p]]
    )
    for h in range(1, half):
        hop = links.next_hop(h, hop, ring_second)
        if h == 1:
            links.relay(in_first, passing_first, moved, relays)
            pass_rows()
    if half == 1:
        links.relay(in_first, passing_first, moved, relays)
        pass_rows()
    for copy in moved:
        copy.wait_recv()

    @pl.loop(0, entries)
    def _(e):
        got_ref[e, upper] = in_first[table_ref[base_slot + e]]

    for copy in hop.values():
        copy.wait_recv()

    @pl.loop(0, entries)
    def _(e):
        got_ref[e, lower] = ring_second[table_ref[base_landed + e]]

    links.finish(arriving, kept[1:])


def swap(steps, collective, table, own_rows, turned):
    x_size, z_size, cores = DIMS
    chunks, per_group, slots, part, width = own_rows.shape
    entries = chunks * turned.shape[1]
    limits = ring_limits()
    landing = 2 * sum(limits)
    peers = x_size * z_size * cores
    block = (part // 2, width)
    copies = 160

    def space(*shape):
        return pltpu.VMEM(shape, jnp.bfloat16)

    scratch = [
        space(entries, part, width),
        space(2, limits[0], *block),
        space(2, limits[0], *block),
        space(landing + x_size * cores, *block),
        space(landing + x_size * cores, *block),
        space(peers, *block),
        space(peers, *block),
        space(peers, *block),
        space(peers, *block),
        space(cores, z_size, *block),
        space(cores, z_size, *block),
        space(2, max(turned.shape[1] // 2, 1), part, width),
        pltpu.VMEM((2, max(per_group // 2, 1), slots, part, width), jnp.float32),
        pltpu.SemaphoreType.DMA((2,)),
        pltpu.SemaphoreType.DMA((copies,)),
        pltpu.SemaphoreType.DMA((copies,)),
    ]
    return pl.pallas_call(
        functools.partial(swap_body, steps),
        out_shape=(
            jax.ShapeDtypeStruct((chunks * per_group, slots, part, width), jnp.float32),
            jax.ShapeDtypeStruct((entries, part, width), jnp.bfloat16),
        ),
        in_specs=[pl.BlockSpec(memory_space=pltpu.SMEM)] + [pl.BlockSpec(memory_space=pl.ANY)] * 2,
        out_specs=[pl.BlockSpec(memory_space=pl.ANY), pl.BlockSpec(memory_space=pltpu.VMEM)],
        scratch_shapes=scratch,
        compiler_params=pltpu.CompilerParams(
            collective_id=collective, has_side_effects=True, vmem_limit_bytes=48 * 2**20
        ),
        name=f"swap_{collective}",
    )(table, own_rows, turned)


def shards(samples, precision_blocks, pair_rows):
    peers = lax.axis_size("var")
    chunks = lax.axis_size("samp")
    rows = samples.shape[0]
    count, slots, width, _ = precision_blocks.shape
    levels = slots - 1
    per_group = count // chunks
    part = width // chunks
    norm_factor = 0.5 / (rows * chunks)

    rung, exchange_table, swap_rung, swap_table = route_tables(pair_rows, peers)
    first_steps, then_steps = ladder(LADDER), ladder(SWAP_LADDER)
    own, fetched = lax.switch(
        rung,
        [
            functools.partial(exchange, steps, i, levels=levels, width=width, chunks=chunks)
            for i, steps in enumerate(first_steps)
        ],
        exchange_table,
        samples,
    )
    group_index = lax.axis_index("samp").astype(jnp.int32).reshape(1)
    own_rows, turned = gradient_terms(group_index, own, fetched, precision_blocks, norm_factor)
    own_rows, turned = lax.switch(
        swap_rung,
        [functools.partial(swap, steps, len(first_steps) + i) for i, steps in enumerate(then_steps)],
        swap_table,
        own_rows,
        turned.reshape(chunks, per_group * levels, part, width),
    )
    return add_turned(own_rows, turned.reshape(count, levels, part, width))


def solution(mesh):
    placed = (P("samp", "var"), P("var", None, None, None), P("var", None))
    return jax.shard_map(
        shards, mesh=mesh, in_specs=placed, out_specs=P("var", None, "samp", None), check_vma=False
    )
```

```python
import functools

import jax
import jax.numpy as jnp
import numpy as np
from jax import lax
from jax.experimental import pallas as pl
from jax.experimental.pallas import tpu as pltpu
from jax.sharding import PartitionSpec as P

DIMS = (4, 8, 2)
CHUNK = 4
SHARES = (5, 7, 4)
LADDER = ((16, 12, 8, 3), (18, 14, 9, 3), (20, 16, 11, 4))
SWAP_LADDER = ((17, 13, 9, 3), (20, 16, 11, 4))
MESH = pl.DeviceIdType.MESH


def ring_limits():
    group = DIMS[0] * DIMS[2]
    half = DIMS[1] // 2
    return tuple(group * (half - h) + (group + 1) // 2 for h in range(1, half + 1))


def offsets_of(limits):
    offsets = [0]
    for limit in limits:
        offsets.append(offsets[-1] + limit)
    return offsets


def ladder(rungs):
    limits = ring_limits()
    steps = [tuple(min(a, b) for a, b in zip(step, limits)) for step in rungs if len(step) == len(limits)]
    return tuple(steps) + (limits,)


def gradient_terms(group_index, own, fetched, precision, norm_factor):
    chunks, levels, per_group, rows, width = fetched.shape
    slots = levels + 1
    part = width // chunks

    def body(index_ref, own_ref, fetched_ref, p_ref, rows_ref, turned_ref):
        totals = [jnp.zeros((width, width), jnp.float32) for _ in range(slots)]
        for s in range(chunks):
            factors = [own_ref[s]] + [fetched_ref[s, k, 0] for k in range(levels)]
            mixed = jnp.zeros((rows, width), jnp.float32)
            for k in range(slots):
                mixed = mixed + jnp.dot(factors[k], p_ref[0, k], preferred_element_type=jnp.float32)
            mixed = mixed.astype(jnp.bfloat16)
            for k in range(slots):
                totals[k] = totals[k] + lax.dot_general(
                    factors[k], mixed, (((0,), (0,)), ((), ())), preferred_element_type=jnp.float32
                )
        for k in range(slots):
            scaled = totals[k] * norm_factor
            turned = scaled.T
            if k == 0:
                scaled = scaled + turned
            for s in range(chunks):
                rows_ref[s, 0, k] = scaled[s * part : (s + 1) * part]
                if k > 0:
                    turned_ref[s, 0, k - 1] = turned[s * part : (s + 1) * part].astype(jnp.bfloat16)

    return pl.pallas_call(
        body,
        out_shape=(
            jax.ShapeDtypeStruct((chunks, per_group, slots, part, width), jnp.float32),
            jax.ShapeDtypeStruct((chunks, per_group, levels, part, width), jnp.bfloat16),
        ),
        grid_spec=pltpu.PrefetchScalarGridSpec(
            num_scalar_prefetch=1,
            grid=(per_group,),
            in_specs=[
                pl.BlockSpec((chunks, rows, width), lambda t, g: (0, 0, t)),
                pl.BlockSpec((chunks, levels, 1, rows, width), lambda t, g: (0, 0, t, 0, 0)),
                pl.BlockSpec((1, slots, width, width), lambda t, g: (g[0] * per_group + t, 0, 0, 0)),
            ],
            out_specs=[
                pl.BlockSpec((chunks, 1, slots, part, width), lambda t, g: (0, t, 0, 0, 0)),
                pl.BlockSpec((chunks, 1, levels, part, width), lambda t, g: (0, t, 0, 0, 0)),
            ],
        ),
        name="gradient_terms",
    )(group_index, own, fetched, precision)


def add_turned(own_rows, turned):
    count, slots, part, width = own_rows.shape
    levels = slots - 1
    group = min(4, count)

    def body(rows_ref, turned_ref, out_ref):
        for i in range(group):
            out_ref[i, 0] = rows_ref[i, 0]
            for k in range(levels):
                out_ref[i, k + 1] = rows_ref[i, k + 1] + turned_ref[i, k].astype(jnp.float32)

    def blocks(slots):
        return pl.BlockSpec((group, slots, part, width), lambda t: (t, 0, 0, 0))

    return pl.pallas_call(
        body,
        out_shape=jax.ShapeDtypeStruct(own_rows.shape, jnp.float32),
        grid=(count // group,),
        in_specs=[blocks(slots), blocks(levels)],
        out_specs=blocks(slots),
        name="add_turned",
    )(own_rows, turned)


def route_tables(pair_rows, peers):
    x_size, z_size, cores = DIMS
    count, slots = pair_rows.shape
    levels = slots - 1
    entries = count * levels
    limits = ring_limits()
    half = z_size // 2
    me = lax.axis_index("var").astype(jnp.int32)
    x, z, core = me // (z_size * cores), (me // cores) % z_size, me % cores
    owner = (pair_rows[:, 1:] // count).reshape(entries)
    px, pz, pcore = owner // (z_size * cores), (owner // cores) % z_size, owner % cores
    cx, cz, cc = jnp.bitwise_xor(px, x), jnp.bitwise_xor(pz, z), jnp.bitwise_xor(pcore, core)
    e_ids = lax.iota(jnp.int32, entries)
    column = e_ids // levels
    earlier = e_ids[None, :] < e_ids[:, None]

    same_cz = cz[None, :] == cz[:, None]
    rank = jnp.sum(jnp.where(same_cz & earlier, 1, 0), axis=1)
    zs = lax.iota(jnp.int32, z_size)[:, None]
    right = (jnp.bitwise_xor(zs, cz[None, :]) - zs) % z_size
    goes_right = (right < half) | ((right == half) & (rank % 2 == 0)[None, :])
    hops = jnp.where(goes_right, right, z_size - right)
    side = jnp.where(right == 0, 2, jnp.where(goes_right, 0, 1))
    order = hops * entries - e_ids[None, :]
    ahead = (side[:, :, None] == side[:, None, :]) & (order[:, None, :] > order[:, :, None])
    place = jnp.sum(jnp.where(ahead, 1, 0), axis=2)

    depth = lax.iota(jnp.int32, half) + 1
    load = [
        jnp.max(jnp.sum(jnp.where((side == s)[:, :, None] & (hops[:, :, None] >= depth), 1, 0), axis=1), axis=0)
        for s in (0, 1)
    ]
    load = jnp.maximum(load[0], load[1])

    def rung_of(rungs):
        steps = jnp.asarray(np.array(ladder(rungs), np.int32))
        fits = jnp.all(steps >= load[None, :], axis=1)
        return jnp.min(jnp.where(fits, lax.iota(jnp.int32, steps.shape[0]), steps.shape[0] - 1))

    def at(table, z_of):
        return jnp.sum(jnp.where(zs == z_of[None, :], table, 0), axis=0)

    z_all = jnp.full((entries,), z)
    my_side, my_place = at(side, z_all), at(place, z_all)
    gathered = (((px - x) % x_size) * cores + cc) * count + column
    length = limits[0]
    spots = lax.iota(jnp.int32, 2 * length + max(x_size * cores, 1))
    spot = jnp.where(my_side == 2, 2 * length + my_place, my_side * length + my_place)
    taken = spots[:, None] == spot[None, :]
    list_column = jnp.sum(jnp.where(taken, column[None, :], 0), axis=1)
    list_gathered = jnp.sum(jnp.where(taken, gathered[None, :], 0), axis=1)

    offsets = offsets_of(limits)
    from_side, from_place, from_hops = at(side, pz), at(place, pz), at(hops, pz)
    start = jnp.zeros((entries,), jnp.int32)
    for h in range(1, half + 1):
        start = jnp.where(from_hops == h, offsets[h - 1], start)
    landed = from_side * offsets[-1] + start + from_place
    landed_first = jnp.where(cz == 0, 2 * offsets[-1] + column, landed)
    landed_second = jnp.where(cz == 0, 2 * offsets[-1] + my_place, landed)
    slot = (cx * cores + cc) * z_size + cz
    at_slot = lax.iota(jnp.int32, peers)[:, None] == slot[None, :]
    slot_first, slot_second, slot_entry = (
        jnp.sum(jnp.where(at_slot, values[None, :], 0), axis=1) for values in (landed_first, landed_second, e_ids)
    )
    list_entry = jnp.sum(jnp.where(taken, e_ids[None, :], 0), axis=1)
    list_slot = jnp.sum(jnp.where(taken, slot[None, :], 0), axis=1)
    exchange_table = jnp.concatenate([list_column, list_gathered, slot_first, slot, landed_second]).astype(jnp.int32)
    swap_table = jnp.concatenate([list_entry, list_slot, slot_second, slot_entry, slot, landed_second]).astype(jnp.int32)
    return rung_of(LADDER), exchange_table, rung_of(SWAP_LADDER), swap_table


class Links:
    def __init__(self, steps, send_sem, recv_sem):
        self.steps, self.send_sem, self.recv_sem = steps, send_sem, recv_sem
        self.x_size, self.z_size, self.cores = DIMS
        self.chunks = lax.axis_size("samp")
        self.offsets = offsets_of(ring_limits())
        self.me = lax.axis_index("var")
        self.group = lax.axis_index("samp")
        self.x = self.me // (self.z_size * self.cores)
        self.z = (self.me // self.cores) % self.z_size
        self.core = self.me % self.cores
        self.copies = []

    def device(self, dx=0, dz=0, dc=0):
        x, z, core = (self.x + dx) % self.x_size, (self.z + dz) % self.z_size, (self.core + dc) % self.cores
        return (self.group, (x * self.z_size + z) * self.cores + core)

    def plane(self, dy):
        return ((self.group + dy) % self.chunks, self.me)

    def remote(self, src, dst, target):
        index = len(self.copies)
        copy = pltpu.make_async_remote_copy(
            src_ref=src, dst_ref=dst, send_sem=self.send_sem.at[index], recv_sem=self.recv_sem.at[index],
            device_id=target, device_id_type=MESH,
        )
        self.copies.append(copy)
        copy.start()
        return copy

    def greet(self):
        barrier = pltpu.get_barrier_semaphore()
        friends = [self.device(dz=1), self.device(dz=-1)]
        if self.x_size > 1:
            friends += [self.device(dx=dx, dc=dc) for dx in (1, -1) for dc in range(self.cores)]
        friends += [self.device(dc=dc) for dc in range(1, self.cores)]
        friends += [self.plane(dy) for dy in range(1, self.chunks)]
        for friend in friends:
            pl.semaphore_signal(barrier, inc=1, device_id=friend, device_id_type=MESH)
        pl.semaphore_wait(barrier, len(friends))

    def first_hop(self, lists, ring, fill):
        sent = {}
        for j, (a, b) in enumerate(ranges(self.steps[0])):
            for s, dz in ((0, 1), (1, -1)):
                @pl.loop(a, b)
                def _(p):
                    fill(s, p)
                landing = ring.at[pl.ds(s * self.offsets[-1] + a, b - a)]
                sent[j, s] = self.remote(lists.at[s, pl.ds(a, b - a)], landing, self.device(dz=dz))
        return sent

    def next_hop(self, h, before, ring):
        sent = {}
        for j, (a, b) in enumerate(ranges(self.steps[h])):
            for s, dz in ((0, 1), (1, -1)):
                before[j, s].wait_recv()
                here = s * self.offsets[-1] + self.offsets[h - 1] + a
                there = s * self.offsets[-1] + self.offsets[h] + a
                sent[j, s] = self.remote(ring.at[pl.ds(here, b - a)], ring.at[pl.ds(there, b - a)], self.device(dz=dz))
        for key, copy in before.items():
            if key not in sent:
                copy.wait_recv()
        return sent

    def across(self, out, landing, passing, fill):
        z_size, cores = self.z_size, self.cores

        def filled(which):
            @pl.loop(which * z_size, (which + 1) * z_size)
            def _(p):
                out[p] = fill(p)
            return pl.ds(which * z_size, z_size)

        arriving, relays = [], []
        if self.x_size > 1:
            for dc in range(cores):
                part = filled(2 * cores + dc)
                relays.append(self.remote(out.at[part], passing.at[dc], self.device(dx=(1, -1)[dc])))
            odd = self.x % 2
            for dc in range(cores):
                part = filled(cores + dc)
                arriving.append(self.remote(out.at[part], landing.at[part], self.device(dx=1 - 2 * odd, dc=dc)))
                part = filled(3 * cores + dc)
                arriving.append(self.remote(out.at[part], landing.at[part], self.device(dx=2 * odd - 1, dc=dc)))
        if cores > 1:
            part = filled(1)
            arriving.append(self.remote(out.at[part], landing.at[part], self.device(dc=1)))

        @pl.loop(0, z_size)
        def _(p):
            landing[p] = fill(p)

        return arriving, relays

    def relay(self, landing, passing, arriving, relays):
        for dc, copy in enumerate(relays):
            copy.wait_recv()
            part = pl.ds((2 * self.cores + dc) * self.z_size, self.z_size)
            arriving.append(self.remote(passing.at[dc], landing.at[part], self.device(dx=(1, -1)[dc], dc=dc)))

    def planes(self, source, landing, passing, pieces):
        arriving, relays = [], []
        four = self.chunks == 4 and pieces == 2
        for dy in range(1, self.chunks):
            target = (self.group + dy) % self.chunks
            if four and dy == 2:
                continue
            for i in range(pieces):
                arriving.append(self.remote(source(target, i), landing(self.group, i), self.plane(dy)))
        if four:
            target = (self.group + 2) % self.chunks
            relays = [
                self.remote(source(target, i), passing(i), self.plane((1, -1)[i])) for i in range(pieces)
            ]

        def pass_on():
            for i, copy in enumerate(relays):
                copy.wait_recv()
                sender = (self.group + (-1, 1)[i]) % self.chunks
                arriving.append(self.remote(passing(i), landing(sender, i), self.plane((1, -1)[i])))

        return arriving, pass_on

    def finish(self, arriving, kept):
        for copy in arriving:
            copy.wait_recv()
        for copy in kept:
            copy.wait()
        for copy in self.copies:
            copy.wait_send()


def ranges(limit):
    return [(a, min(a + CHUNK, limit)) for a in range(0, limit, CHUNK)]


def exchange_body(steps, parts, table_ref, x_ref, own_ref, fetched_ref, *scratch):
    lists, rings, columns, relayed = (scratch[i * len(parts) : (i + 1) * len(parts)] for i in range(4))
    slots_out, slots_in, passing, stage, local_sem, send_sem, recv_sem = scratch[4 * len(parts) :]
    links = Links(steps, send_sem, recv_sem)
    x_size, z_size, cores = DIMS
    chunks = links.chunks
    rows, total = x_ref.shape
    width = fetched_ref.shape[-1]
    count = total // width
    levels = fetched_ref.shape[1]
    per_group = fetched_ref.shape[2]
    entries = count * levels
    half = z_size // 2
    length = ring_limits()[0]
    tail = 2 * links.offsets[-1]
    local = x_size * cores
    base_gathered = 2 * length + local
    base_source = 2 * base_gathered
    base_slot = base_source + x_size * z_size * cores
    base_landed = base_slot + entries
    own_first = columns[0]

    links.greet()

    def column_of(index):
        return pl.ds(pl.multiple_of(index * width, width), width)

    def split_columns(i):
        first, size = parts[i]

        @pl.loop(0, count)
        def _(t):
            columns[i][t] = x_ref[first : first + size, column_of(t)]

    split_columns(0)

    def fill_first(s, p):
        lists[0][s, p] = own_first[table_ref[s * length + p]]

    hop = links.first_hop(lists[0], rings[0], fill_first)

    class Gather:
        def __init__(self, i):
            self.columns, self.slabs, self.near, self.far = columns[i], [], [], []

        def slab(self, dx, dc, first=0, size=count):
            return self.columns.at[pl.ds((dx * cores + dc) * count + first, size)]

        def start(self):
            if x_size > 1:
                self.near = [
                    links.remote(self.slab(0, 0), self.slab(x_size - 1, 0), links.device(dx=1)),
                    links.remote(self.slab(0, 0), self.slab(1, 0), links.device(dx=-1)),
                ]
            if cores > 1:
                self.slabs.append(links.remote(self.slab(0, 0), self.slab(0, 1), links.device(dc=1)))

        def share(self, dx):
            if cores > 1:
                self.slabs.append(links.remote(self.slab(dx, 0), self.slab(dx, 1), links.device(dc=1)))

        def go_far(self):
            some = count // 2
            for copy in self.near:
                copy.wait_recv()
            if self.near:
                self.far = [
                    links.remote(self.slab(x_size - 1, 0, 0, some), self.slab(2, 0, 0, some), links.device(dx=1)),
                    links.remote(self.slab(1, 0, some, some), self.slab(2, 0, some, some), links.device(dx=-1)),
                ]
                self.share(1)
                self.share(x_size - 1)

        def finish(self):
            for copy in self.far:
                copy.wait_recv()
            if self.far:
                self.share(2)

        def wait(self):
            for copy in self.slabs:
                copy.wait_recv()

    gathers = {}
    for i in range(1, len(parts)):
        split_columns(i)
        gathers[i] = Gather(i)
    gathers[1].start()

    wide = total // chunks

    def quarter(which):
        return x_ref.at[:, pl.ds(pl.multiple_of(which * wide, width), wide)]

    arriving = [
        links.remote(quarter((links.group + dy) % chunks), own_ref.at[links.group], links.plane(dy))
        for dy in range(1, chunks)
    ]
    kept = [pltpu.make_async_copy(quarter(links.group), own_ref.at[links.group], local_sem.at[0])]
    kept[0].start()

    @pl.loop(0, count)
    def _(t):
        rings[0][tail + t] = own_first[t]

    def stage_part(i, load):
        rows_of = pl.ds(*parts[i])
        for k in range(levels):
            @pl.loop(0, count)
            def _(t):
                stage[t // per_group, k * per_group + t % per_group, rows_of] = load(t * levels + k)
        landed, pass_on = links.planes(
            lambda target, k: stage.at[target, pl.ds(k * per_group, per_group), rows_of],
            lambda sender, k: fetched_ref.at[sender, k, :, rows_of],
            lambda k: relayed[i].at[k],
            levels,
        )
        for k in range(levels):
            copy = pltpu.make_async_copy(
                stage.at[links.group, pl.ds(k * per_group, per_group), rows_of],
                fetched_ref.at[links.group, k, :, rows_of],
                local_sem.at[1 + i * levels + k],
            )
            copy.start()
            kept.append(copy)
        return landed, pass_on

    def go_round(i):
        def fill(s, p):
            lists[i][s, p] = columns[i][table_ref[base_gathered + s * length + p]]

        sent = links.first_hop(lists[i], rings[i], fill)

        @pl.loop(0, local)
        def _(p):
            rings[i][tail + p] = columns[i][table_ref[base_gathered + 2 * length + p]]

        return sent

    def land(i):
        return stage_part(i, lambda e: rings[i][table_ref[base_landed + e]])

    for h in range(1, half):
        hop = links.next_hop(h, hop, rings[0])
        if h == 1:
            gathers[1].go_far()
            if 2 in gathers:
                gathers[2].start()
        if h == 2 or half <= 2:
            gathers[1].finish()
    if 2 in gathers:
        gathers[2].go_far()
    gathers[1].wait()
    last, hop = hop, go_round(1)
    for copy in last.values():
        copy.wait_recv()
    moved, relays = links.across(slots_out, slots_in, passing, lambda p: rings[0][table_ref[base_source + p]])

    def first_along_y():
        for copy in moved:
            copy.wait_recv()
        return stage_part(0, lambda e: slots_in[table_ref[base_slot + e]])

    landed = {}
    for h in range(1, half):
        hop = links.next_hop(h, hop, rings[1])
        if h == 1:
            links.relay(slots_in, passing, moved, relays)
            if 2 in gathers:
                gathers[2].finish()
        if h == 2:
            landed[0] = first_along_y()
    if half <= 2:
        landed[0] = first_along_y()
    landed[0][1]()
    if 2 in gathers:
        gathers[2].wait()
        last, hop = hop, go_round(2)
        for copy in last.values():
            copy.wait_recv()
        landed[1] = land(1)
        for h in range(1, half):
            hop = links.next_hop(h, hop, rings[2])
            if h == 1:
                landed[1][1]()
    for copy in hop.values():
        copy.wait_recv()
    final = len(parts) - 1
    landed[final] = land(final)
    landed[final][1]()
    links.finish(arriving + [copy for copies, _ in landed.values() for copy in copies], kept)


def exchange(steps, collective, table, samples, levels, width, chunks):
    x_size, z_size, cores = DIMS
    rows, total = samples.shape
    count = total // width
    per_group = count // chunks
    sixteenth = rows // 16
    sizes = tuple(sixteenth * share for share in SHARES)
    parts = tuple((sum(sizes[:i]), size) for i, size in enumerate(sizes))
    limits = ring_limits()
    landing = 2 * sum(limits)
    peers = x_size * z_size * cores
    copies = 200

    def space(*shape):
        return pltpu.VMEM(shape, jnp.bfloat16)

    scratch = (
        [space(2, limits[0], size, width) for size in sizes]
        + [space(landing + (x_size * cores if i else count), size, width) for i, size in enumerate(sizes)]
        + [space((x_size * cores if i else 1) * count, size, width) for i, size in enumerate(sizes)]
        + [space(levels, per_group, size, width) for size in sizes]
        + [
            space(peers, sizes[0], width),
            space(peers, sizes[0], width),
            space(cores, z_size, sizes[0], width),
            space(chunks, levels * per_group, rows, width),
            pltpu.SemaphoreType.DMA((1 + len(parts) * levels,)),
            pltpu.SemaphoreType.DMA((copies,)),
            pltpu.SemaphoreType.DMA((copies,)),
        ]
    )
    return pl.pallas_call(
        functools.partial(exchange_body, steps, parts),
        out_shape=(
            jax.ShapeDtypeStruct((chunks, rows, total // chunks), jnp.bfloat16),
            jax.ShapeDtypeStruct((chunks, levels, per_group, rows, width), jnp.bfloat16),
        ),
        in_specs=[pl.BlockSpec(memory_space=pltpu.SMEM), pl.BlockSpec(memory_space=pltpu.VMEM)],
        out_specs=[pl.BlockSpec(memory_space=pl.ANY)] * 2,
        scratch_shapes=scratch,
        compiler_params=pltpu.CompilerParams(
            collective_id=collective, has_side_effects=True, vmem_limit_bytes=61 * 2**20
        ),
        name=f"exchange_{collective}",
    )(table, samples)


def swap_body(steps, table_ref, rows_ref, turned_ref, out_rows_ref, got_ref, mine_upper, mine_lower, list_first, list_second, ring_first,
              ring_second, out_first, in_first, out_second, in_second, passing_first, passing_second, passing_upper,
              passing_lower, passing_rows, local_sem, send_sem, recv_sem):
    links = Links(steps, send_sem, recv_sem)
    x_size, z_size, cores = DIMS
    chunks = links.chunks
    per_group = rows_ref.shape[1]
    entries, part, width = got_ref.shape
    each = entries // chunks
    half_part = part // 2
    half = z_size // 2
    length = ring_limits()[0]
    tail = 2 * links.offsets[-1]
    local = x_size * cores
    peers = x_size * z_size * cores
    base_slots = 2 * length + local
    base_source = 2 * base_slots
    base_entry = base_source + peers
    base_slot = base_entry + peers
    base_landed = base_slot + entries
    upper, lower = pl.ds(0, half_part), pl.ds(half_part, half_part)

    links.greet()
    kept = []

    def keep(src, dst):
        copy = pltpu.make_async_copy(src, dst, local_sem.at[len(kept)])
        copy.start()
        kept.append(copy)

    some = each // 2

    def turned_planes(rows, mine, passing):
        keep(turned_ref.at[links.group, :, rows], mine.at[pl.ds(links.group * each, each)])
        return links.planes(
            lambda target, i: turned_ref.at[target, pl.ds(i * some, some), rows],
            lambda sender, i: mine.at[pl.ds(sender * each + i * some, some)],
            lambda i: passing.at[i],
            2,
        )

    arrived_upper, pass_upper = turned_planes(upper, mine_upper, passing_upper)
    pass_upper()
    arrived_lower, pass_lower = turned_planes(lower, mine_lower, passing_lower)
    for copy in arrived_upper:
        copy.wait_recv()
    kept[0].wait()

    def fill_first(s, p):
        list_first[s, p] = mine_upper[table_ref[s * length + p]]

    hop = links.first_hop(list_first, ring_first, fill_first)
    pass_lower()
    keep(rows_ref.at[links.group], out_rows_ref.at[pl.ds(links.group * per_group, per_group)])
    few = per_group // 2 if per_group > 1 else 1
    arriving, pass_rows = links.planes(
        lambda target, i: rows_ref.at[target, pl.ds(i * few, few)],
        lambda sender, i: out_rows_ref.at[pl.ds(sender * per_group + i * few, few)],
        lambda i: passing_rows.at[i],
        per_group // few,
    )
    for copy in arrived_lower:
        copy.wait_recv()
    kept[1].wait()
    moved, relays = links.across(
        out_second, in_second, passing_second, lambda p: mine_lower[table_ref[base_entry + p]]
    )

    @pl.loop(0, local)
    def _(p):
        ring_first[tail + p] = mine_upper[table_ref[2 * length + p]]

    for h in range(1, half):
        hop = links.next_hop(h, hop, ring_first)
        if h == 1:
            links.relay(in_second, passing_second, moved, relays)
    if half == 1:
        links.relay(in_second, passing_second, moved, relays)
    for copy in moved:
        copy.wait_recv()

    def fill_second(s, p):
        list_second[s, p] = in_second[table_ref[base_slots + s * length + p]]

    last = hop
    hop = links.first_hop(list_second, ring_second, fill_second)

    @pl.loop(0, local)
    def _(p):
        ring_second[tail + p] = in_second[table_ref[base_slots + 2 * length + p]]

    for copy in last.values():
        copy.wait_recv()
    moved, relays = links.across(
        out_first, in_first, passing_first, lambda p: ring_first[table_ref[base_source + p]]
    )
    for h in range(1, half):
        hop = links.next_hop(h, hop, ring_second)
        if h == 1:
            links.relay(in_first, passing_first, moved, relays)
            pass_rows()
    if half == 1:
        links.relay(in_first, passing_first, moved, relays)
        pass_rows()
    for copy in moved:
        copy.wait_recv()

    @pl.loop(0, entries)
    def _(e):
        got_ref[e, upper] = in_first[table_ref[base_slot + e]]

    for copy in hop.values():
        copy.wait_recv()

    @pl.loop(0, entries)
    def _(e):
        got_ref[e, lower] = ring_second[table_ref[base_landed + e]]

    links.finish(arriving, kept[2:])


def swap(steps, collective, table, own_rows, turned):
    x_size, z_size, cores = DIMS
    chunks, per_group, slots, part, width = own_rows.shape
    entries = chunks * turned.shape[1]
    limits = ring_limits()
    landing = 2 * sum(limits)
    peers = x_size * z_size * cores
    block = (part // 2, width)
    copies = 160

    def space(*shape):
        return pltpu.VMEM(shape, jnp.bfloat16)

    scratch = [
        space(entries, *block),
        space(entries, *block),
        space(2, limits[0], *block),
        space(2, limits[0], *block),
        space(landing + x_size * cores, *block),
        space(landing + x_size * cores, *block),
        space(peers, *block),
        space(peers, *block),
        space(peers, *block),
        space(peers, *block),
        space(cores, z_size, *block),
        space(cores, z_size, *block),
        space(2, max(turned.shape[1] // 2, 1), *block),
        space(2, max(turned.shape[1] // 2, 1), *block),
        pltpu.VMEM((2, max(per_group // 2, 1), slots, part, width), jnp.float32),
        pltpu.SemaphoreType.DMA((3,)),
        pltpu.SemaphoreType.DMA((copies,)),
        pltpu.SemaphoreType.DMA((copies,)),
    ]
    return pl.pallas_call(
        functools.partial(swap_body, steps),
        out_shape=(
            jax.ShapeDtypeStruct((chunks * per_group, slots, part, width), jnp.float32),
            jax.ShapeDtypeStruct((entries, part, width), jnp.bfloat16),
        ),
        in_specs=[pl.BlockSpec(memory_space=pltpu.SMEM)] + [pl.BlockSpec(memory_space=pl.ANY)] * 2,
        out_specs=[pl.BlockSpec(memory_space=pl.ANY), pl.BlockSpec(memory_space=pltpu.VMEM)],
        scratch_shapes=scratch,
        compiler_params=pltpu.CompilerParams(
            collective_id=collective, has_side_effects=True, vmem_limit_bytes=48 * 2**20
        ),
        name=f"swap_{collective}",
    )(table, own_rows, turned)


def shards(samples, precision_blocks, pair_rows):
    peers = lax.axis_size("var")
    chunks = lax.axis_size("samp")
    rows = samples.shape[0]
    count, slots, width, _ = precision_blocks.shape
    levels = slots - 1
    per_group = count // chunks
    part = width // chunks
    norm_factor = 0.5 / (rows * chunks)

    rung, exchange_table, swap_rung, swap_table = route_tables(pair_rows, peers)
    first_steps, then_steps = ladder(LADDER), ladder(SWAP_LADDER)
    own, fetched = lax.switch(
        rung,
        [
            functools.partial(exchange, steps, i, levels=levels, width=width, chunks=chunks)
            for i, steps in enumerate(first_steps)
        ],
        exchange_table,
        samples,
    )
    group_index = lax.axis_index("samp").astype(jnp.int32).reshape(1)
    own_rows, turned = gradient_terms(group_index, own, fetched, precision_blocks, norm_factor)
    own_rows, turned = lax.switch(
        swap_rung,
        [functools.partial(swap, steps, len(first_steps) + i) for i, steps in enumerate(then_steps)],
        swap_table,
        own_rows,
        turned.reshape(chunks, per_group * levels, part, width),
    )
    return add_turned(own_rows, turned.reshape(count, levels, part, width))


def solution(mesh):
    placed = (P("samp", "var"), P("var", None, None, None), P("var", None))
    return jax.shard_map(
        shards, mesh=mesh, in_specs=placed, out_specs=P("var", None, "samp", None), check_vma=False
    )
```

```python
import functools

import jax
import jax.numpy as jnp
import numpy as np
from jax import lax
from jax.experimental import pallas as pl
from jax.experimental.pallas import tpu as pltpu
from jax.sharding import PartitionSpec as P

DIMS = (4, 8, 2)
CHUNK = 4
SHARES = (6, 6, 4)
LADDER = ((16, 11, 7, 2), (16, 12, 8, 3), (17, 13, 8, 3), (18, 14, 9, 3), (20, 16, 11, 4))
SWAP_LADDER = ((17, 13, 9, 3), (20, 16, 11, 4))
MESH = pl.DeviceIdType.MESH


def ring_limits():
    group = DIMS[0] * DIMS[2]
    half = DIMS[1] // 2
    return tuple(group * (half - h) + (group + 1) // 2 for h in range(1, half + 1))


def offsets_of(limits):
    offsets = [0]
    for limit in limits:
        offsets.append(offsets[-1] + limit)
    return offsets


def ladder(rungs):
    limits = ring_limits()
    steps = [tuple(min(a, b) for a, b in zip(step, limits)) for step in rungs if len(step) == len(limits)]
    return tuple(steps) + (limits,)


def gradient_terms(group_index, own, fetched, precision, norm_factor):
    chunks, levels, per_group, rows, width = fetched.shape
    slots = levels + 1
    part = width // chunks

    def body(index_ref, own_ref, fetched_ref, p_ref, rows_ref, turned_ref):
        totals = [jnp.zeros((width, width), jnp.float32) for _ in range(slots)]
        for s in range(chunks):
            factors = [own_ref[s]] + [fetched_ref[s, k, 0] for k in range(levels)]
            mixed = jnp.zeros((rows, width), jnp.float32)
            for k in range(slots):
                mixed = mixed + jnp.dot(factors[k], p_ref[0, k], preferred_element_type=jnp.float32)
            mixed = mixed.astype(jnp.bfloat16)
            for k in range(slots):
                totals[k] = totals[k] + lax.dot_general(
                    factors[k], mixed, (((0,), (0,)), ((), ())), preferred_element_type=jnp.float32
                )
        for k in range(slots):
            scaled = totals[k] * norm_factor
            turned = scaled.T
            if k == 0:
                scaled = scaled + turned
            for s in range(chunks):
                rows_ref[s, 0, k] = scaled[s * part : (s + 1) * part]
                if k > 0:
                    turned_ref[s, 0, k - 1] = turned[s * part : (s + 1) * part].astype(jnp.bfloat16)

    return pl.pallas_call(
        body,
        out_shape=(
            jax.ShapeDtypeStruct((chunks, per_group, slots, part, width), jnp.float32),
            jax.ShapeDtypeStruct((chunks, per_group, levels, part, width), jnp.bfloat16),
        ),
        grid_spec=pltpu.PrefetchScalarGridSpec(
            num_scalar_prefetch=1,
            grid=(per_group,),
            in_specs=[
                pl.BlockSpec((chunks, rows, width), lambda t, g: (0, 0, t)),
                pl.BlockSpec((chunks, levels, 1, rows, width), lambda t, g: (0, 0, t, 0, 0)),
                pl.BlockSpec((1, slots, width, width), lambda t, g: (g[0] * per_group + t, 0, 0, 0)),
            ],
            out_specs=[
                pl.BlockSpec((chunks, 1, slots, part, width), lambda t, g: (0, t, 0, 0, 0)),
                pl.BlockSpec((chunks, 1, levels, part, width), lambda t, g: (0, t, 0, 0, 0)),
            ],
        ),
        name="gradient_terms",
    )(group_index, own, fetched, precision)


def add_turned(own_rows, turned):
    count, slots, part, width = own_rows.shape
    levels = slots - 1
    group = min(4, count)

    def body(rows_ref, turned_ref, out_ref):
        for i in range(group):
            out_ref[i, 0] = rows_ref[i, 0]
            for k in range(levels):
                out_ref[i, k + 1] = rows_ref[i, k + 1] + turned_ref[i, k].astype(jnp.float32)

    def blocks(slots):
        return pl.BlockSpec((group, slots, part, width), lambda t: (t, 0, 0, 0))

    return pl.pallas_call(
        body,
        out_shape=jax.ShapeDtypeStruct(own_rows.shape, jnp.float32),
        grid=(count // group,),
        in_specs=[blocks(slots), blocks(levels)],
        out_specs=blocks(slots),
        name="add_turned",
    )(own_rows, turned)


def route_tables(pair_rows, peers):
    x_size, z_size, cores = DIMS
    count, slots = pair_rows.shape
    levels = slots - 1
    entries = count * levels
    limits = ring_limits()
    half = z_size // 2
    me = lax.axis_index("var").astype(jnp.int32)
    x, z, core = me // (z_size * cores), (me // cores) % z_size, me % cores
    owner = (pair_rows[:, 1:] // count).reshape(entries)
    px, pz, pcore = owner // (z_size * cores), (owner // cores) % z_size, owner % cores
    cx, cz, cc = jnp.bitwise_xor(px, x), jnp.bitwise_xor(pz, z), jnp.bitwise_xor(pcore, core)
    e_ids = lax.iota(jnp.int32, entries)
    column = e_ids // levels
    earlier = e_ids[None, :] < e_ids[:, None]

    same_cz = cz[None, :] == cz[:, None]
    rank = jnp.sum(jnp.where(same_cz & earlier, 1, 0), axis=1)
    zs = lax.iota(jnp.int32, z_size)[:, None]
    right = (jnp.bitwise_xor(zs, cz[None, :]) - zs) % z_size
    goes_right = (right < half) | ((right == half) & (rank % 2 == 0)[None, :])
    hops = jnp.where(goes_right, right, z_size - right)
    side = jnp.where(right == 0, 2, jnp.where(goes_right, 0, 1))
    order = hops * entries - e_ids[None, :]
    ahead = (side[:, :, None] == side[:, None, :]) & (order[:, None, :] > order[:, :, None])
    place = jnp.sum(jnp.where(ahead, 1, 0), axis=2)

    depth = lax.iota(jnp.int32, half) + 1
    load = [
        jnp.max(jnp.sum(jnp.where((side == s)[:, :, None] & (hops[:, :, None] >= depth), 1, 0), axis=1), axis=0)
        for s in (0, 1)
    ]
    load = jnp.maximum(load[0], load[1])

    def rung_of(rungs):
        steps = jnp.asarray(np.array(ladder(rungs), np.int32))
        fits = jnp.all(steps >= load[None, :], axis=1)
        return jnp.min(jnp.where(fits, lax.iota(jnp.int32, steps.shape[0]), steps.shape[0] - 1))

    def at(table, z_of):
        return jnp.sum(jnp.where(zs == z_of[None, :], table, 0), axis=0)

    z_all = jnp.full((entries,), z)
    my_side, my_place = at(side, z_all), at(place, z_all)
    gathered = (((px - x) % x_size) * cores + cc) * count + column
    length = limits[0]
    spots = lax.iota(jnp.int32, 2 * length + max(x_size * cores, 1))
    spot = jnp.where(my_side == 2, 2 * length + my_place, my_side * length + my_place)
    taken = spots[:, None] == spot[None, :]
    list_column = jnp.sum(jnp.where(taken, column[None, :], 0), axis=1)
    list_gathered = jnp.sum(jnp.where(taken, gathered[None, :], 0), axis=1)

    offsets = offsets_of(limits)
    from_side, from_place, from_hops = at(side, pz), at(place, pz), at(hops, pz)
    start = jnp.zeros((entries,), jnp.int32)
    for h in range(1, half + 1):
        start = jnp.where(from_hops == h, offsets[h - 1], start)
    landed = from_side * offsets[-1] + start + from_place
    landed_first = jnp.where(cz == 0, 2 * offsets[-1] + column, landed)
    landed_second = jnp.where(cz == 0, 2 * offsets[-1] + my_place, landed)
    slot = (cx * cores + cc) * z_size + cz
    at_slot = lax.iota(jnp.int32, peers)[:, None] == slot[None, :]
    slot_first, slot_second, slot_entry = (
        jnp.sum(jnp.where(at_slot, values[None, :], 0), axis=1) for values in (landed_first, landed_second, e_ids)
    )
    list_entry = jnp.sum(jnp.where(taken, e_ids[None, :], 0), axis=1)
    list_slot = jnp.sum(jnp.where(taken, slot[None, :], 0), axis=1)
    exchange_table = jnp.concatenate([list_column, list_gathered, slot_first, slot, landed_second]).astype(jnp.int32)
    swap_table = jnp.concatenate([list_entry, list_slot, slot_second, slot_entry, slot, landed_second]).astype(jnp.int32)
    return rung_of(LADDER), exchange_table, rung_of(SWAP_LADDER), swap_table


class Links:
    def __init__(self, steps, send_sem, recv_sem):
        self.steps, self.send_sem, self.recv_sem = steps, send_sem, recv_sem
        self.x_size, self.z_size, self.cores = DIMS
        self.chunks = lax.axis_size("samp")
        self.offsets = offsets_of(ring_limits())
        self.me = lax.axis_index("var")
        self.group = lax.axis_index("samp")
        self.x = self.me // (self.z_size * self.cores)
        self.z = (self.me // self.cores) % self.z_size
        self.core = self.me % self.cores
        self.copies = []

    def device(self, dx=0, dz=0, dc=0):
        x, z, core = (self.x + dx) % self.x_size, (self.z + dz) % self.z_size, (self.core + dc) % self.cores
        return (self.group, (x * self.z_size + z) * self.cores + core)

    def plane(self, dy):
        return ((self.group + dy) % self.chunks, self.me)

    def remote(self, src, dst, target):
        index = len(self.copies)
        copy = pltpu.make_async_remote_copy(
            src_ref=src, dst_ref=dst, send_sem=self.send_sem.at[index], recv_sem=self.recv_sem.at[index],
            device_id=target, device_id_type=MESH,
        )
        self.copies.append(copy)
        copy.start()
        return copy

    def greet(self):
        barrier = pltpu.get_barrier_semaphore()
        friends = [self.device(dz=1), self.device(dz=-1)]
        if self.x_size > 1:
            friends += [self.device(dx=dx, dc=dc) for dx in (1, -1) for dc in range(self.cores)]
        friends += [self.device(dc=dc) for dc in range(1, self.cores)]
        friends += [self.plane(dy) for dy in range(1, self.chunks)]
        for friend in friends:
            pl.semaphore_signal(barrier, inc=1, device_id=friend, device_id_type=MESH)
        pl.semaphore_wait(barrier, len(friends))

    def first_hop(self, lists, ring, fill):
        sent = {}
        for j, (a, b) in enumerate(ranges(self.steps[0])):
            for s, dz in ((0, 1), (1, -1)):
                @pl.loop(a, b)
                def _(p):
                    fill(s, p)
                landing = ring.at[pl.ds(s * self.offsets[-1] + a, b - a)]
                sent[j, s] = self.remote(lists.at[s, pl.ds(a, b - a)], landing, self.device(dz=dz))
        return sent

    def next_hop(self, h, before, ring):
        sent = {}
        for j, (a, b) in enumerate(ranges(self.steps[h])):
            for s, dz in ((0, 1), (1, -1)):
                before[j, s].wait_recv()
                here = s * self.offsets[-1] + self.offsets[h - 1] + a
                there = s * self.offsets[-1] + self.offsets[h] + a
                sent[j, s] = self.remote(ring.at[pl.ds(here, b - a)], ring.at[pl.ds(there, b - a)], self.device(dz=dz))
        for key, copy in before.items():
            if key not in sent:
                copy.wait_recv()
        return sent

    def across(self, out, landing, passing, fill):
        z_size, cores = self.z_size, self.cores

        def filled(which):
            @pl.loop(which * z_size, (which + 1) * z_size)
            def _(p):
                out[p] = fill(p)
            return pl.ds(which * z_size, z_size)

        arriving, relays = [], []
        if self.x_size > 1:
            for dc in range(cores):
                part = filled(2 * cores + dc)
                relays.append(self.remote(out.at[part], passing.at[dc], self.device(dx=(1, -1)[dc])))
            odd = self.x % 2
            for dc in range(cores):
                part = filled(cores + dc)
                arriving.append(self.remote(out.at[part], landing.at[part], self.device(dx=1 - 2 * odd, dc=dc)))
                part = filled(3 * cores + dc)
                arriving.append(self.remote(out.at[part], landing.at[part], self.device(dx=2 * odd - 1, dc=dc)))
        if cores > 1:
            part = filled(1)
            arriving.append(self.remote(out.at[part], landing.at[part], self.device(dc=1)))

        @pl.loop(0, z_size)
        def _(p):
            landing[p] = fill(p)

        return arriving, relays

    def relay(self, landing, passing, arriving, relays):
        for dc, copy in enumerate(relays):
            copy.wait_recv()
            part = pl.ds((2 * self.cores + dc) * self.z_size, self.z_size)
            arriving.append(self.remote(passing.at[dc], landing.at[part], self.device(dx=(1, -1)[dc], dc=dc)))

    def planes(self, source, landing, passing, pieces):
        arriving, relays = [], []
        four = self.chunks == 4 and pieces == 2
        for dy in range(1, self.chunks):
            target = (self.group + dy) % self.chunks
            if four and dy == 2:
                continue
            for i in range(pieces):
                arriving.append(self.remote(source(target, i), landing(self.group, i), self.plane(dy)))
        if four:
            target = (self.group + 2) % self.chunks
            relays = [
                self.remote(source(target, i), passing(i), self.plane((1, -1)[i])) for i in range(pieces)
            ]

        def pass_on():
            for i, copy in enumerate(relays):
                copy.wait_recv()
                sender = (self.group + (-1, 1)[i]) % self.chunks
                arriving.append(self.remote(passing(i), landing(sender, i), self.plane((1, -1)[i])))

        return arriving, pass_on

    def finish(self, arriving, kept):
        for copy in arriving:
            copy.wait_recv()
        for copy in kept:
            copy.wait()
        for copy in self.copies:
            copy.wait_send()


def ranges(limit):
    return [(a, min(a + CHUNK, limit)) for a in range(0, limit, CHUNK)]


def exchange_body(steps, parts, table_ref, x_ref, own_ref, fetched_ref, *scratch):
    lists, rings, columns, relayed = (scratch[i * len(parts) : (i + 1) * len(parts)] for i in range(4))
    slots_out, slots_in, passing, stage, local_sem, send_sem, recv_sem = scratch[4 * len(parts) :]
    links = Links(steps, send_sem, recv_sem)
    x_size, z_size, cores = DIMS
    chunks = links.chunks
    rows, total = x_ref.shape
    width = fetched_ref.shape[-1]
    count = total // width
    levels = fetched_ref.shape[1]
    per_group = fetched_ref.shape[2]
    entries = count * levels
    half = z_size // 2
    length = ring_limits()[0]
    tail = 2 * links.offsets[-1]
    local = x_size * cores
    base_gathered = 2 * length + local
    base_source = 2 * base_gathered
    base_slot = base_source + x_size * z_size * cores
    base_landed = base_slot + entries
    own_first = columns[0]

    links.greet()

    def column_of(index):
        return pl.ds(pl.multiple_of(index * width, width), width)

    def split_columns(i):
        first, size = parts[i]

        @pl.loop(0, count)
        def _(t):
            columns[i][t] = x_ref[first : first + size, column_of(t)]

    split_columns(0)

    def fill_first(s, p):
        lists[0][s, p] = own_first[table_ref[s * length + p]]

    hop = links.first_hop(lists[0], rings[0], fill_first)

    class Gather:
        def __init__(self, i):
            self.columns, self.slabs, self.near, self.far = columns[i], [], [], []

        def slab(self, dx, dc, first=0, size=count):
            return self.columns.at[pl.ds((dx * cores + dc) * count + first, size)]

        def start(self):
            if x_size > 1:
                self.near = [
                    links.remote(self.slab(0, 0), self.slab(x_size - 1, 0), links.device(dx=1)),
                    links.remote(self.slab(0, 0), self.slab(1, 0), links.device(dx=-1)),
                ]
            if cores > 1:
                self.slabs.append(links.remote(self.slab(0, 0), self.slab(0, 1), links.device(dc=1)))

        def share(self, dx):
            if cores > 1:
                self.slabs.append(links.remote(self.slab(dx, 0), self.slab(dx, 1), links.device(dc=1)))

        def go_far(self):
            some = count // 2
            for copy in self.near:
                copy.wait_recv()
            if self.near:
                self.far = [
                    links.remote(self.slab(x_size - 1, 0, 0, some), self.slab(2, 0, 0, some), links.device(dx=1)),
                    links.remote(self.slab(1, 0, some, some), self.slab(2, 0, some, some), links.device(dx=-1)),
                ]
                self.share(1)
                self.share(x_size - 1)

        def finish(self):
            for copy in self.far:
                copy.wait_recv()
            if self.far:
                self.share(2)

        def wait(self):
            for copy in self.slabs:
                copy.wait_recv()

    gathers = {}
    for i in range(1, len(parts)):
        split_columns(i)
        gathers[i] = Gather(i)
    gathers[1].start()

    wide = total // chunks

    def quarter(which):
        return x_ref.at[:, pl.ds(pl.multiple_of(which * wide, width), wide)]

    arriving = [
        links.remote(quarter((links.group + dy) % chunks), own_ref.at[links.group], links.plane(dy))
        for dy in range(1, chunks)
    ]
    kept = [pltpu.make_async_copy(quarter(links.group), own_ref.at[links.group], local_sem.at[0])]
    kept[0].start()

    @pl.loop(0, count)
    def _(t):
        rings[0][tail + t] = own_first[t]

    def stage_part(i, load):
        rows_of = pl.ds(*parts[i])
        for k in range(levels):
            @pl.loop(0, count)
            def _(t):
                stage[t // per_group, k * per_group + t % per_group, rows_of] = load(t * levels + k)
        landed, pass_on = links.planes(
            lambda target, k: stage.at[target, pl.ds(k * per_group, per_group), rows_of],
            lambda sender, k: fetched_ref.at[sender, k, :, rows_of],
            lambda k: relayed[i].at[k],
            levels,
        )
        for k in range(levels):
            copy = pltpu.make_async_copy(
                stage.at[links.group, pl.ds(k * per_group, per_group), rows_of],
                fetched_ref.at[links.group, k, :, rows_of],
                local_sem.at[1 + i * levels + k],
            )
            copy.start()
            kept.append(copy)
        return landed, pass_on

    def go_round(i):
        def fill(s, p):
            lists[i][s, p] = columns[i][table_ref[base_gathered + s * length + p]]

        sent = links.first_hop(lists[i], rings[i], fill)

        @pl.loop(0, local)
        def _(p):
            rings[i][tail + p] = columns[i][table_ref[base_gathered + 2 * length + p]]

        return sent

    def land(i):
        return stage_part(i, lambda e: rings[i][table_ref[base_landed + e]])

    for h in range(1, half):
        hop = links.next_hop(h, hop, rings[0])
        if h == 1:
            gathers[1].go_far()
            if 2 in gathers:
                gathers[2].start()
        if h == 2 or half <= 2:
            gathers[1].finish()
    if 2 in gathers:
        gathers[2].go_far()
    gathers[1].wait()
    last, hop = hop, go_round(1)
    for copy in last.values():
        copy.wait_recv()
    moved, relays = links.across(slots_out, slots_in, passing, lambda p: rings[0][table_ref[base_source + p]])

    def first_along_y():
        for copy in moved:
            copy.wait_recv()
        return stage_part(0, lambda e: slots_in[table_ref[base_slot + e]])

    landed = {}
    for h in range(1, half):
        hop = links.next_hop(h, hop, rings[1])
        if h == 1:
            links.relay(slots_in, passing, moved, relays)
            if 2 in gathers:
                gathers[2].finish()
    if 2 not in gathers:
        landed[0] = first_along_y()
        landed[0][1]()
    if 2 in gathers:
        gathers[2].wait()
        last, hop = hop, go_round(2)
        landed[0] = first_along_y()
        for copy in last.values():
            copy.wait_recv()
        landed[1] = land(1)
        landed[0][1]()
        for h in range(1, half):
            hop = links.next_hop(h, hop, rings[2])
            if h == 1:
                landed[1][1]()
    for copy in hop.values():
        copy.wait_recv()
    final = len(parts) - 1
    landed[final] = land(final)
    landed[final][1]()
    links.finish(arriving + [copy for copies, _ in landed.values() for copy in copies], kept)


def exchange(steps, collective, table, samples, levels, width, chunks):
    x_size, z_size, cores = DIMS
    rows, total = samples.shape
    count = total // width
    per_group = count // chunks
    sixteenth = rows // 16
    sizes = tuple(sixteenth * share for share in SHARES)
    parts = tuple((sum(sizes[:i]), size) for i, size in enumerate(sizes))
    limits = ring_limits()
    landing = 2 * sum(limits)
    peers = x_size * z_size * cores
    copies = 200

    def space(*shape):
        return pltpu.VMEM(shape, jnp.bfloat16)

    scratch = (
        [space(2, limits[0], size, width) for size in sizes]
        + [space(landing + (x_size * cores if i else count), size, width) for i, size in enumerate(sizes)]
        + [space((x_size * cores if i else 1) * count, size, width) for i, size in enumerate(sizes)]
        + [space(levels, per_group, size, width) for size in sizes]
        + [
            space(peers, sizes[0], width),
            space(peers, sizes[0], width),
            space(cores, z_size, sizes[0], width),
            space(chunks, levels * per_group, rows, width),
            pltpu.SemaphoreType.DMA((1 + len(parts) * levels,)),
            pltpu.SemaphoreType.DMA((copies,)),
            pltpu.SemaphoreType.DMA((copies,)),
        ]
    )
    return pl.pallas_call(
        functools.partial(exchange_body, steps, parts),
        out_shape=(
            jax.ShapeDtypeStruct((chunks, rows, total // chunks), jnp.bfloat16),
            jax.ShapeDtypeStruct((chunks, levels, per_group, rows, width), jnp.bfloat16),
        ),
        in_specs=[pl.BlockSpec(memory_space=pltpu.SMEM), pl.BlockSpec(memory_space=pltpu.VMEM)],
        out_specs=[pl.BlockSpec(memory_space=pl.ANY)] * 2,
        scratch_shapes=scratch,
        compiler_params=pltpu.CompilerParams(
            collective_id=collective, has_side_effects=True, vmem_limit_bytes=61 * 2**20
        ),
        name=f"exchange_{collective}",
    )(table, samples)


def swap_body(steps, table_ref, rows_ref, turned_ref, out_rows_ref, got_ref, mine_upper, mine_lower, list_first, list_second, ring_first,
              ring_second, out_first, in_first, out_second, in_second, passing_first, passing_second, passing_upper,
              passing_lower, passing_rows, local_sem, send_sem, recv_sem):
    links = Links(steps, send_sem, recv_sem)
    x_size, z_size, cores = DIMS
    chunks = links.chunks
    per_group = rows_ref.shape[1]
    entries, part, width = got_ref.shape
    each = entries // chunks
    half_part = part // 2
    half = z_size // 2
    length = ring_limits()[0]
    tail = 2 * links.offsets[-1]
    local = x_size * cores
    peers = x_size * z_size * cores
    base_slots = 2 * length + local
    base_source = 2 * base_slots
    base_entry = base_source + peers
    base_slot = base_entry + peers
    base_landed = base_slot + entries
    upper, lower = pl.ds(0, half_part), pl.ds(half_part, half_part)

    links.greet()
    kept = []

    def keep(src, dst):
        copy = pltpu.make_async_copy(src, dst, local_sem.at[len(kept)])
        copy.start()
        kept.append(copy)

    some = each // 2

    def turned_planes(rows, mine, passing):
        keep(turned_ref.at[links.group, :, rows], mine.at[pl.ds(links.group * each, each)])
        return links.planes(
            lambda target, i: turned_ref.at[target, pl.ds(i * some, some), rows],
            lambda sender, i: mine.at[pl.ds(sender * each + i * some, some)],
            lambda i: passing.at[i],
            2,
        )

    arrived_upper, pass_upper = turned_planes(upper, mine_upper, passing_upper)
    pass_upper()
    arrived_lower, pass_lower = turned_planes(lower, mine_lower, passing_lower)
    for copy in arrived_upper:
        copy.wait_recv()
    kept[0].wait()

    def fill_first(s, p):
        list_first[s, p] = mine_upper[table_ref[s * length + p]]

    hop = links.first_hop(list_first, ring_first, fill_first)
    pass_lower()
    keep(rows_ref.at[links.group], out_rows_ref.at[pl.ds(links.group * per_group, per_group)])
    few = per_group // 2 if per_group > 1 else 1
    arriving, pass_rows = links.planes(
        lambda target, i: rows_ref.at[target, pl.ds(i * few, few)],
        lambda sender, i: out_rows_ref.at[pl.ds(sender * per_group + i * few, few)],
        lambda i: passing_rows.at[i],
        per_group // few,
    )
    for copy in arrived_lower:
        copy.wait_recv()
    kept[1].wait()
    moved, relays = links.across(
        out_second, in_second, passing_second, lambda p: mine_lower[table_ref[base_entry + p]]
    )

    @pl.loop(0, local)
    def _(p):
        ring_first[tail + p] = mine_upper[table_ref[2 * length + p]]

    for h in range(1, half):
        hop = links.next_hop(h, hop, ring_first)
        if h == 1:
            links.relay(in_second, passing_second, moved, relays)
    if half == 1:
        links.relay(in_second, passing_second, moved, relays)
    for copy in moved:
        copy.wait_recv()

    def fill_second(s, p):
        list_second[s, p] = in_second[table_ref[base_slots + s * length + p]]

    last = hop
    hop = links.first_hop(list_second, ring_second, fill_second)

    @pl.loop(0, local)
    def _(p):
        ring_second[tail + p] = in_second[table_ref[base_slots + 2 * length + p]]

    for copy in last.values():
        copy.wait_recv()
    moved, relays = links.across(
        out_first, in_first, passing_first, lambda p: ring_first[table_ref[base_source + p]]
    )
    for h in range(1, half):
        hop = links.next_hop(h, hop, ring_second)
        if h == 1:
            links.relay(in_first, passing_first, moved, relays)
            pass_rows()
    if half == 1:
        links.relay(in_first, passing_first, moved, relays)
        pass_rows()
    for copy in moved:
        copy.wait_recv()

    @pl.loop(0, entries)
    def _(e):
        got_ref[e, upper] = in_first[table_ref[base_slot + e]]

    for copy in hop.values():
        copy.wait_recv()

    @pl.loop(0, entries)
    def _(e):
        got_ref[e, lower] = ring_second[table_ref[base_landed + e]]

    links.finish(arriving, kept[2:])


def swap(steps, collective, table, own_rows, turned):
    x_size, z_size, cores = DIMS
    chunks, per_group, slots, part, width = own_rows.shape
    entries = chunks * turned.shape[1]
    limits = ring_limits()
    landing = 2 * sum(limits)
    peers = x_size * z_size * cores
    block = (part // 2, width)
    copies = 160

    def space(*shape):
        return pltpu.VMEM(shape, jnp.bfloat16)

    scratch = [
        space(entries, *block),
        space(entries, *block),
        space(2, limits[0], *block),
        space(2, limits[0], *block),
        space(landing + x_size * cores, *block),
        space(landing + x_size * cores, *block),
        space(peers, *block),
        space(peers, *block),
        space(peers, *block),
        space(peers, *block),
        space(cores, z_size, *block),
        space(cores, z_size, *block),
        space(2, max(turned.shape[1] // 2, 1), *block),
        space(2, max(turned.shape[1] // 2, 1), *block),
        pltpu.VMEM((2, max(per_group // 2, 1), slots, part, width), jnp.float32),
        pltpu.SemaphoreType.DMA((3,)),
        pltpu.SemaphoreType.DMA((copies,)),
        pltpu.SemaphoreType.DMA((copies,)),
    ]
    return pl.pallas_call(
        functools.partial(swap_body, steps),
        out_shape=(
            jax.ShapeDtypeStruct((chunks * per_group, slots, part, width), jnp.float32),
            jax.ShapeDtypeStruct((entries, part, width), jnp.bfloat16),
        ),
        in_specs=[pl.BlockSpec(memory_space=pltpu.SMEM)] + [pl.BlockSpec(memory_space=pl.ANY)] * 2,
        out_specs=[pl.BlockSpec(memory_space=pl.ANY), pl.BlockSpec(memory_space=pltpu.VMEM)],
        scratch_shapes=scratch,
        compiler_params=pltpu.CompilerParams(
            collective_id=collective, has_side_effects=True, vmem_limit_bytes=48 * 2**20
        ),
        name=f"swap_{collective}",
    )(table, own_rows, turned)


def shards(samples, precision_blocks, pair_rows):
    peers = lax.axis_size("var")
    chunks = lax.axis_size("samp")
    rows = samples.shape[0]
    count, slots, width, _ = precision_blocks.shape
    levels = slots - 1
    per_group = count // chunks
    part = width // chunks
    norm_factor = 0.5 / (rows * chunks)

    rung, exchange_table, swap_rung, swap_table = route_tables(pair_rows, peers)
    first_steps, then_steps = ladder(LADDER), ladder(SWAP_LADDER)
    own, fetched = lax.switch(
        rung,
        [
            functools.partial(exchange, steps, i, levels=levels, width=width, chunks=chunks)
            for i, steps in enumerate(first_steps)
        ],
        exchange_table,
        samples,
    )
    group_index = lax.axis_index("samp").astype(jnp.int32).reshape(1)
    own_rows, turned = gradient_terms(group_index, own, fetched, precision_blocks, norm_factor)
    own_rows, turned = lax.switch(
        swap_rung,
        [functools.partial(swap, steps, len(first_steps) + i) for i, steps in enumerate(then_steps)],
        swap_table,
        own_rows,
        turned.reshape(chunks, per_group * levels, part, width),
    )
    return add_turned(own_rows, turned.reshape(count, levels, part, width))


def solution(mesh):
    placed = (P("samp", "var"), P("var", None, None, None), P("var", None))
    return jax.shard_map(
        shards, mesh=mesh, in_specs=placed, out_specs=P("var", None, "samp", None), check_vma=False
    )
```
